128 devices in a mesh: ty: 8 (over y, core), tx: 16 (over x, z).
Axes of the slice: x: 4, y: 4, z: 4, core: 2. Of those that a mesh axis runs over, the one named last changes fastest.
Arguments:
- node_state: bfloat16 [8192, 256], P(('ty', 'tx')), may hold values from -6 to 6
- edge_state: bfloat16 [8192, 50, 256], P(('ty', 'tx')), may hold values from -6 to 6
- noisy_edges: float32 [8192, 50], P(('ty', 'tx')), may hold values from -1 to 1
- timestep: int32 [1], replicated, may hold values from 1 to 999
- neighbors: int32 [8192, 50], P(('ty', 'tx')), may hold values from -1 to 8191, as said below
- mirror_src: int32 [8192, 50], P(('ty', 'tx')), may hold values from -1 to 3327, as said below
- send_rows: int32 [128, 8, 16], P(('ty', 'tx')), may hold values from -1 to 3199, as said below
- node_own: bfloat16 [3, 256, 512], replicated, may hold values from -0.375 to 0.375
- node_nbr: bfloat16 [3, 256, 512], replicated, may hold values from -0.375 to 0.375
- edge_weight: bfloat16 [3, 256, 256], replicated, may hold values from -0.375 to 0.375
- noise_embed: float32 [256], replicated, may hold values from -6 to 6
- time_embed: float32 [256, 256], replicated, may hold values from -0.375 to 0.375
- time_layer: float32 [3, 256, 256], replicated, may hold values from -0.375 to 0.375
Outputs:
- node_out: bfloat16 [8192, 256], P(('ty', 'tx'))
- edge_out: bfloat16 [8192, 50, 256], P(('ty', 'tx'))
The draws below stay inside these ranges and needn't reach their ends.
Inputs may be any that keep to these rules, and one draw needn't show every extreme that they name: `neighbors`: every listed neighbour lies in the city's own tile or one of the 8 tiles adjacent to it (diagonals too); padding slots hold -1. mirror_src[i, k] is -1 or an index of lookup (the tile's own edge rows, then incoming); the row it names is the edge from neighbors[i, k] back to city i. An index of 3200 or more, d * 16 + p past the own rows, names the p-th row from offset d. send_rows[s, d] lists, -1 for unused entries, the rows of tile s that the tile at offset minus d from s reads as its offset d rows, in order; at most 16 rows for one pair of adjacent tiles, and in every draw some tile reads exactly 16 from each adjacent tile and they from it.
All inputs are finite; a program needn't handle non-finite values.
Results may differ from the reference program's by a relative error of at most 0.0055.
Values may be sent and summed in bfloat16 or wider, within the bound.
A program may use at most 64 MiB of HBM per device.

```python
import math
import jax
import jax.numpy as jnp
from jax import lax

WIDTH = 256
K = 50
LAYERS = 3
C_DEV = 64
GRID_Y = 8
GRID_X = 16
TILES = 128
CITIES = 8192
CAP = 16


def direction_list_drawn():
    return [(step_y, step_x) for step_y in (-1, 0, 1) for step_x in (-1, 0, 1) if step_y != 0 or step_x != 0]


def permutations(key, count, length):
    keys_all = jax.random.split(key, count)
    return jax.vmap(lambda member: jax.random.permutation(member, length))(keys_all).astype(jnp.int32)


def inverse_of(ordering):
    return jnp.argsort(ordering, axis=-1).astype(jnp.int32)


def build_graph(key):
    base_key = jax.random.fold_in(key, 7101)
    tile_count = GRID_Y * GRID_X
    tile_ids = jnp.arange(tile_count, dtype=jnp.int32)
    tile_y = tile_ids // GRID_X
    tile_x = tile_ids % GRID_X
    directions = direction_list_drawn()
    sigma = permutations(jax.random.fold_in(base_key, 1), tile_count * 16, C_DEV).reshape(tile_count, 16, C_DEV)
    sigma_inv = inverse_of(sigma)
    offset_city = (tile_ids * C_DEV)[:, None, None]
    intra_nbr = jnp.stack([sigma, sigma_inv], axis=-1).transpose(0, 2, 1, 3).reshape(tile_count, C_DEV, 32) + offset_city
    intra_slot = jnp.broadcast_to(jnp.arange(32, dtype=jnp.int32) ^ 1, (tile_count, C_DEV, 32))
    first_perm = permutations(jax.random.fold_in(base_key, 2), tile_count * 4, C_DEV).reshape(tile_count, 4, C_DEV)
    second_perm = permutations(jax.random.fold_in(base_key, 3), tile_count * 4, C_DEV).reshape(tile_count, 4, C_DEV)
    raw_counts = jax.random.randint(jax.random.fold_in(base_key, 4), (tile_count, 4), CAP // 8, CAP // 2 + 1).astype(jnp.int32)
    full_tile = jax.random.randint(jax.random.fold_in(base_key, 5), (), 0, tile_count).astype(jnp.int32)
    partners = []
    insides = []
    for direction, (step_y, step_x) in enumerate(directions):
        near_y = tile_y + step_y
        near_x = tile_x + step_x
        inside = (near_y >= 0) & (near_y < GRID_Y) & (near_x >= 0) & (near_x < GRID_X)
        partners.append(jnp.clip(near_y, 0, GRID_Y - 1) * GRID_X + jnp.clip(near_x, 0, GRID_X - 1))
        insides.append(inside)
    count_list = []
    for direction in range(4):
        involves = (tile_ids == full_tile) | (partners[direction] == full_tile) & insides[direction]
        count_list.append(jnp.where(insides[direction], jnp.where(involves, CAP, raw_counts[:, direction]), 0))
    pair_counts = jnp.stack(count_list, axis=1)
    cross_nbr = []
    cross_dir = []
    cross_pos = []
    cross_slot = []
    recv_global = []
    for direction in range(8):
        partner = partners[direction]
        if direction < 4:
            own_order = first_perm[:, direction]
            far_order = second_perm[:, direction]
            count = pair_counts[:, direction]
        else:
            own_order = second_perm[partner, 7 - direction]
            far_order = first_perm[partner, 7 - direction]
            count = jnp.where(insides[direction], pair_counts[partner, 7 - direction], 0)
        rank = inverse_of(own_order)
        active = rank < count[:, None]
        far_city = jnp.take_along_axis(far_order, rank, axis=1)
        cross_nbr.append(jnp.where(active, partner[:, None] * C_DEV + far_city, -1))
        cross_dir.append(jnp.where(active, direction, -2))
        cross_pos.append(rank)
        cross_slot.append(jnp.full((tile_count, C_DEV), 32 + 7 - direction, jnp.int32))
        place = jnp.arange(CAP, dtype=jnp.int32)[None, :]
        recv_global.append(jnp.where(place < count[:, None], partner[:, None] * C_DEV + far_order[:, :CAP], -1))
    jump_y = jax.random.randint(jax.random.fold_in(base_key, 6), (tile_count, C_DEV, 8), -1, 2)
    jump_x = jax.random.randint(jax.random.fold_in(base_key, 7), (tile_count, C_DEV, 8), -1, 2)
    far_y = jnp.clip(tile_y[:, None, None] + jump_y, 0, GRID_Y - 1)
    far_x = jnp.clip(tile_x[:, None, None] + jump_x, 0, GRID_X - 1)
    pick_city = jax.random.randint(jax.random.fold_in(base_key, 8), (tile_count, C_DEV, 8), 0, C_DEV)
    oneway_nbr = ((far_y * GRID_X + far_x) * C_DEV + pick_city).astype(jnp.int32)
    minus_two = jnp.full((tile_count, C_DEV, 2), -1, jnp.int32)
    minus_ten = jnp.full((tile_count, C_DEV, 10), -1, jnp.int32)
    zeros_ten = jnp.zeros((tile_count, C_DEV, 10), jnp.int32)
    cross_nbr_all = jnp.stack(cross_nbr, axis=-1).astype(jnp.int32)
    base_nbr = jnp.concatenate([intra_nbr, cross_nbr_all, oneway_nbr, minus_two], axis=-1)
    base_city = jnp.concatenate([intra_nbr, cross_nbr_all, minus_ten], axis=-1)
    base_slot = jnp.concatenate([intra_slot, jnp.stack(cross_slot, axis=-1), zeros_ten], axis=-1)
    base_dir = jnp.concatenate([jnp.full((tile_count, C_DEV, 32), -1, jnp.int32), jnp.stack(cross_dir, axis=-1).astype(jnp.int32), jnp.full((tile_count, C_DEV, 10), -2, jnp.int32)], axis=-1)
    base_pos = jnp.concatenate([jnp.zeros((tile_count, C_DEV, 32), jnp.int32), jnp.stack(cross_pos, axis=-1), zeros_ten], axis=-1)
    slot_order = permutations(jax.random.fold_in(base_key, 9), tile_count * C_DEV, K).reshape(tile_count, C_DEV, K)
    slot_place = inverse_of(slot_order).reshape(tile_count * C_DEV, K)
    neighbors = jnp.take_along_axis(base_nbr, slot_order, axis=-1)
    safe_city = jnp.maximum(base_city, 0).reshape(-1)
    mirror_final = slot_place[safe_city, base_slot.reshape(-1)].reshape(tile_count, C_DEV, K)
    intra_row = safe_city.reshape(tile_count, C_DEV, K) % C_DEV * K + mirror_final
    cross_row = C_DEV * K + jnp.maximum(base_dir, 0) * CAP + base_pos
    mirror_base = jnp.where(base_dir == -1, intra_row, jnp.where(base_dir >= 0, cross_row, -1))
    mirror_src = jnp.take_along_axis(mirror_base, slot_order, axis=-1)
    send_list = []
    for direction, (step_y, step_x) in enumerate(directions):
        wanted = recv_global[direction]
        safe_want = jnp.maximum(wanted, 0)
        row_of = safe_want % C_DEV * K + slot_place[safe_want, 32 + 7 - direction]
        recv_rows = jnp.where(wanted >= 0, row_of, -1)
        back_y = tile_y - step_y
        back_x = tile_x - step_x
        back_inside = (back_y >= 0) & (back_y < GRID_Y) & (back_x >= 0) & (back_x < GRID_X)
        back_tile = jnp.clip(back_y, 0, GRID_Y - 1) * GRID_X + jnp.clip(back_x, 0, GRID_X - 1)
        send_list.append(jnp.where(back_inside[:, None], recv_rows[back_tile], -1))
    send_rows = jnp.stack(send_list, axis=1).astype(jnp.int32)
    return (neighbors.reshape(tile_count * C_DEV, K).astype(jnp.int32), mirror_src.reshape(tile_count * C_DEV, K).astype(jnp.int32), send_rows)


def draw_neighbors(key, part):
    return build_graph(key)[0]


def draw_mirror_src(key, part):
    return build_graph(key)[1]


def draw_send_rows(key, part):
    return build_graph(key)[2]


def levels(key, dims, cuts, least, top_value):
    def one(dim, blocks):
        heights = jax.random.uniform(jax.random.fold_in(jax.random.fold_in(key, 6), dim), (blocks,), jnp.float32, least / len(cuts), top_value / len(cuts))
        return jnp.repeat(jnp.exp(heights), dims[dim] // blocks).reshape((-1,) + (1,) * (len(dims) - dim - 1))

    factor_of = one(*cuts[0])
    for cut in cuts[1:]:
        factor_of = factor_of * one(*cut)
    return factor_of


def centred(rng, extent, width, limit, cuts=(), kind=jnp.bfloat16):
    entries = jax.random.normal(rng, extent, jnp.float32) * width
    if len(cuts) > 0:
        entries = levels(rng, extent, cuts, -0.22, 0.18) * entries
    return jnp.clip(entries, min=-limit, max=limit).astype(kind)


def setup_inputs(seed: int = 0) -> dict:
    key_of = jax.random.split(jax.random.key(seed), 14)
    return {
        "node_state": centred(key_of[0], (CITIES, WIDTH), 1.0, 6.0, ((0, 128),)),
        "edge_state": centred(key_of[1], (CITIES, K, WIDTH), 1.0, 6.0, ((0, 128),)),
        "noisy_edges": jnp.clip(jax.random.uniform(key_of[2], (CITIES, K), jnp.float32, -1.0, 1.0) * levels(key_of[2], (CITIES, K), ((0, 128),), -0.4, 0.0), -1.0, 1.0),
        "timestep": jax.random.randint(key_of[3], (1,), 1, 1000).astype(jnp.int32),
        "neighbors": draw_neighbors(jax.random.fold_in(key_of[13], 71), 0),
        "mirror_src": draw_mirror_src(jax.random.fold_in(key_of[13], 71), 0),
        "send_rows": draw_send_rows(jax.random.fold_in(key_of[13], 71), 0),
        "node_own": centred(key_of[7], (LAYERS, WIDTH, 2 * WIDTH), WIDTH ** -0.5, 0.375),
        "node_nbr": centred(key_of[8], (LAYERS, WIDTH, 2 * WIDTH), WIDTH ** -0.5, 0.375),
        "edge_weight": centred(key_of[9], (LAYERS, WIDTH, WIDTH), WIDTH ** -0.5, 0.375),
        "noise_embed": centred(key_of[10], (WIDTH,), 1.0, 6.0, (), jnp.float32),
        "time_embed": centred(key_of[11], (WIDTH, WIDTH), WIDTH ** -0.5, 0.375, (), jnp.float32),
        "time_layer": centred(key_of[12], (LAYERS, WIDTH, WIDTH), WIDTH ** -0.5, 0.375, (), jnp.float32),
    }


def direction_list():
    return [(step_y, step_x) for step_y in (-1, 0, 1) for step_x in (-1, 0, 1) if step_y != 0 or step_x != 0]

def layer_norm(values):
    centered = values - lax.optimization_barrier(jnp.mean(values, axis=-1, keepdims=True))
    spread = lax.optimization_barrier(jnp.mean(centered * centered, axis=-1, keepdims=True))
    return centered * lax.rsqrt(spread + 1e-05)

def time_hidden_of(timestep, time_embed):
    features = time_embed.shape[0]
    half_width = features // 2
    frequency = jnp.exp(-math.log(10000.0) * jnp.arange(half_width, dtype=jnp.float32) / half_width)
    phases = timestep[0].astype(jnp.float32) * frequency
    embedding = jnp.concatenate([jnp.cos(phases), jnp.sin(phases)])[None, :]
    return jax.nn.relu(jnp.dot(embedding, time_embed, precision=lax.Precision.HIGHEST))

def edge_update(node_rows, averaged, own_proj, picked, is_valid, noisy, noise_embed, time_row, weight):
    cities = picked.shape[0]
    slot_count = picked.shape[1]
    features = averaged.shape[1]
    valid3 = is_valid[:, :, None]
    mixed_rows = jnp.dot(averaged, weight, preferred_element_type=jnp.float32).reshape(cities, slot_count, features)
    picked_src = picked[:, :, :features].astype(jnp.float32)
    picked_msg = picked[:, :, features:].astype(jnp.float32)
    pre_gate = mixed_rows + own_proj[:, None, :features] + jnp.where(valid3, picked_src, 0.0)
    pre_gate = pre_gate + noisy[:, :, None] * noise_embed + time_row
    gate_vals = jnp.where(valid3, jax.nn.sigmoid(pre_gate), 0.0)
    gathered = lax.optimization_barrier(jnp.sum(gate_vals * picked_msg, axis=1))
    node_next = (node_rows.astype(jnp.float32) + jax.nn.relu(layer_norm(own_proj[:, features:] + gathered))).astype(jnp.bfloat16)
    averaged3 = averaged.reshape(cities, slot_count, features).astype(jnp.float32)
    edge_next = jnp.where(valid3, averaged3 + jax.nn.relu(layer_norm(pre_gate)), 0.0).astype(jnp.bfloat16)
    return (node_next, edge_next)

def take_rows(source_rows, positions):
    return jnp.take(source_rows, positions, axis=0)

def reference(node_state, edge_state, noisy_edges, timestep, neighbors, mirror_src, send_rows, node_own, node_nbr, edge_weight, noise_embed, time_embed, time_layer):
    row_count = C_DEV * K
    hidden_time = time_hidden_of(timestep, time_embed)
    valid_all = (neighbors >= 0).reshape(TILES, C_DEV, K)
    safe_all = jnp.where(neighbors >= 0, neighbors, 0).reshape(TILES, row_count)
    mirror_all = mirror_src.reshape(TILES, row_count)
    noisy_all = noisy_edges.reshape(TILES, C_DEV, K)
    send_live = (send_rows >= 0).reshape(TILES, 8 * CAP)
    send_safe = jnp.maximum(send_rows, 0).reshape(TILES, 8 * CAP)
    node_rows = node_state.reshape(TILES, C_DEV, WIDTH)
    edge_rows = edge_state.reshape(TILES, row_count, WIDTH)
    for layer_at in range(LAYERS):
        time_row = jnp.dot(hidden_time, time_layer[layer_at], precision=lax.Precision.HIGHEST)
        projected = jnp.dot(node_rows.reshape(CITIES, WIDTH), node_nbr[layer_at], preferred_element_type=jnp.float32).astype(jnp.bfloat16)
        outbound = jax.vmap(take_rows)(edge_rows, send_safe)
        outbound = jnp.where(send_live[:, :, None], outbound, jnp.zeros_like(outbound))
        padded = jnp.pad(outbound.reshape(GRID_Y, GRID_X, 8, CAP, WIDTH), ((1, 1), (1, 1), (0, 0), (0, 0), (0, 0)))
        pieces = [padded[1 + step_y:1 + step_y + GRID_Y, 1 + step_x:1 + step_x + GRID_X, direction] for direction, (step_y, step_x) in enumerate(direction_list())]
        incoming = jnp.stack(pieces, axis=2).reshape(TILES, 8 * CAP, WIDTH)
        own_weight = node_own[layer_at]
        edge_w = edge_weight[layer_at]

        def tile_step(members):
            node_tile, edge_tile, mirror_tile, safe_tile, valid_tile, noisy_tile, incoming_tile = members
            lookup = jnp.concatenate([edge_tile, incoming_tile], axis=0)
            partner = jnp.take(lookup, jnp.maximum(mirror_tile, 0), axis=0)
            averaged = jnp.where((mirror_tile >= 0)[:, None], (edge_tile.astype(jnp.float32) + partner.astype(jnp.float32)) * 0.5, edge_tile.astype(jnp.float32)).astype(jnp.bfloat16)
            own_proj = jnp.dot(node_tile, own_weight, preferred_element_type=jnp.float32)
            picked = jnp.take(projected, safe_tile, axis=0).reshape(C_DEV, K, 2 * WIDTH)
            return edge_update(node_tile, averaged, own_proj, picked, valid_tile, noisy_tile, noise_embed, time_row, edge_w)
        node_rows, edge_next = lax.map(tile_step, (node_rows, edge_rows, mirror_all, safe_all, valid_all, noisy_all, incoming))
        edge_rows = edge_next.reshape(TILES, row_count, WIDTH)
    return (node_rows.reshape(CITIES, WIDTH), edge_rows.reshape(CITIES, K, WIDTH))
```

```python
import functools
import math

import jax
import jax.numpy as jnp
from jax import lax
from jax.experimental import pallas as pl
from jax.experimental.pallas import tpu as pltpu
from jax.sharding import PartitionSpec as P

LAYERS = 3
CITIES = 64
SLOTS = 50
WIDTH = 256
ROWS = CITIES * SLOTS
CAP = 16
INCOMING = 8 * CAP
LOOKUP = ROWS + INCOMING
EARLY = 3072
PICK = 768
CHUNK = 640
MESH = pl.DeviceIdType.MESH
F32 = jnp.float32
BF16 = jnp.bfloat16
OFFSETS = [(y, x) for y in (-1, 0, 1) for x in (-1, 0, 1) if (y, x) != (0, 0)]


def norm(values):
    centered = values - jnp.mean(values, axis=-1, keepdims=True)
    spread = jnp.mean(centered * centered, axis=-1, keepdims=True)
    return centered * lax.rsqrt(spread + 1e-05)


def split(values):
    high = values.astype(BF16).astype(F32)
    return high, values - high


def dot(a, b):
    return jnp.dot(a, b, preferred_element_type=F32)


def column(row, lanes):
    n = row.shape[1]
    eye = lax.broadcasted_iota(jnp.int32, (n, n), 0) == lanes
    return jnp.sum(jnp.where(eye, jnp.broadcast_to(row, (n, n)), 0.0), axis=1, keepdims=True)


def one_hot_tiles(index, value, tiles):
    n = index.shape[0]
    lanes = lax.broadcasted_iota(jnp.int32, (n, 128), 1)
    low = jnp.where(lanes == (index & 127), value, 0.0).astype(BF16)
    high = jnp.broadcast_to((index >> 7).astype(F32), (n, 128)).astype(BF16)
    zero = jnp.zeros((n, 128), BF16)
    return [jnp.where(high == jnp.asarray(t, BF16), low, zero) for t in range(tiles)]


def kernel(
    grid_y,
    grid_x,
    node_ref,
    edge_hbm,
    noisy_ref,
    nbr_ref,
    mirror_ref,
    send_ref,
    own_w,
    nbr_w,
    edge_w,
    noise_ref,
    emb_ref,
    time_embed,
    time_layer,
    node_out,
    edge_out,
    mix,
    pick,
    edges,
    averaged_early,
    picked_from,
    send_hot,
    fields,
    hist,
    nodes_in,
    edges_in,
    edges_sent,
    send_sem,
    recv_sem,
    copy_sem,
):
    here_y = lax.axis_index("ty")
    here_x = lax.axis_index("tx")
    targets = [
        (lax.rem(here_y - y + grid_y, grid_y), lax.rem(here_x - x + grid_x, grid_x))
        for y, x in OFFSETS
    ]
    barrier = pltpu.get_barrier_semaphore()
    for target in targets:
        pl.semaphore_signal(barrier, inc=1, device_id=target, device_id_type=MESH)

    load = pltpu.make_async_copy(edge_hbm, edges.at[0, pl.ds(0, ROWS)], copy_sem)
    load.start()

    def node_copy(layer, d, source):
        return pltpu.make_async_remote_copy(
            src_ref=source,
            dst_ref=nodes_in.at[layer, pl.ds(d * CITIES, CITIES)],
            send_sem=send_sem.at[layer, d],
            recv_sem=recv_sem.at[layer, d],
            device_id=targets[d],
            device_id_type=MESH,
        )

    def edge_copy(layer, d):
        return pltpu.make_async_remote_copy(
            src_ref=edges_sent.at[layer, pl.ds(d * CAP, CAP)],
            dst_ref=edges_in.at[layer, pl.ds(d * CAP, CAP)],
            send_sem=send_sem.at[layer, 8 + d],
            recv_sem=recv_sem.at[layer, 8 + d],
            device_id=targets[d],
            device_id_type=MESH,
        )

    nbr = nbr_ref[...]
    valid = nbr >= 0
    safe = jnp.maximum(nbr, 0)
    tile = safe >> 6
    rel = ((tile >> 4) - here_y + 1) * 3 + (tile & 15) - here_x + 1
    block = jnp.where(rel < 4, rel, jnp.where(rel == 4, 8, rel - 1))
    pick_at = jnp.where(valid, block * CITIES + (safe & 63), -1)
    mirror = mirror_ref[...]
    city = (mirror * 5243) >> 18
    local = (mirror - city * SLOTS) * CITIES + city
    came = (mirror - ROWS) >> 4
    came = came + jnp.where(came >= 4, 1, 0)
    came_y = (came * 11) >> 5
    from_y = here_y + came_y - 1
    from_x = here_x + (came - 3 * came_y) - 1
    inside = (from_y >= 0) & (from_y < grid_y) & (from_x >= 0) & (from_x < grid_x)
    remote = jnp.where(inside, mirror, -1)
    has = mirror >= 0
    partner_at = jnp.where(has, jnp.where(mirror >= ROWS, remote, local), -1)
    packed = (partner_at + 1) + jnp.where(has, 4096, 0) + (pick_at + 1) * 8192
    fields[...] = packed.astype(F32)

    hist[0] = node_ref[...]
    sends = send_ref[0]
    sent_city = (sends * 5243) >> 18
    sent_at = jnp.where(sends >= 0, (sends - sent_city * SLOTS) * CITIES + sent_city, -1)
    sent_at = sent_at.astype(F32)
    lanes16 = lax.broadcasted_iota(jnp.int32, (CAP, CAP), 1)
    for d in range(8):
        index = column(sent_at[d : d + 1], lanes16).astype(jnp.int32)
        for t, hot in enumerate(one_hot_tiles(index, 1.0, ROWS // 128)):
            send_hot[pl.ds(d * CAP, CAP), pl.ds(t * 128, 128)] = hot

    pl.semaphore_wait(barrier, 8)
    for d in range(8):
        node_copy(0, d, node_ref).start()
    load.wait()
    edges_sent[0] = dot(send_hot[...], edges[0, pl.ds(0, ROWS)]).astype(BF16)

    lanes64 = lax.broadcasted_iota(jnp.int32, (CITIES, CITIES), 1)
    lanes = lax.broadcasted_iota(jnp.int32, (CITIES, 128), 1)
    rows = lax.broadcasted_iota(jnp.int32, (CITIES, 128), 0)

    def build(k, carry):
        at = pl.ds(pl.multiple_of(k * CITIES, CITIES), CITIES)
        packed = column(fields[pl.ds(k, 1)], lanes64).astype(jnp.int32)
        noise = column(noisy_ref[pl.ds(k, 1)], lanes64)
        pick_at = (packed >> 13) - 1
        valid = pick_at >= 0
        has = ((packed >> 12) & 1) > 0
        partner_at = jnp.where(valid, (packed & 4095) - 1, -1)
        own_part = jnp.where(valid, jnp.where(has, 0.5, 1.0), 0.0)
        for t, hot in enumerate(one_hot_tiles(partner_at, 0.5, LOOKUP // 128)):
            mix[at, pl.ds(t * 128, 128)] = hot
        own_at = pl.ds(pl.multiple_of((k // 2) * 128, 128), 128)
        own = jnp.where(lanes == rows + lax.rem(k, 2) * CITIES, own_part, 0.0)
        mix[at, own_at] = (mix[at, own_at].astype(F32) + own).astype(BF16)
        hots = one_hot_tiles(pick_at, 1.0, 5)
        live = jnp.where(valid, 1.0, 0.0)
        for t in range(4):
            pick[at, pl.ds(t * 128, 128)] = hots[t]
        high = jnp.where(lanes == rows + CITIES, live, 0.0)
        pick[at, pl.ds(512, 128)] = (hots[4].astype(F32) + high).astype(BF16)
        noise_high, noise_low = split(noise * live)
        low = jnp.where(lanes == rows, live, 0.0)
        low = jnp.where((lanes == 64) | (lanes == 66), noise_high, low)
        low = jnp.where(lanes == 65, noise_low, low)
        pick[at, pl.ds(640, 128)] = low.astype(BF16)
        return carry

    lax.fori_loop(0, SLOTS, build, 0)
    for d in range(8):
        edge_copy(0, d).start()

    noise_high, noise_low = split(noise_ref[...])
    which = lax.broadcasted_iota(jnp.int32, (CITIES, WIDTH), 0)
    noise_rows = jnp.where(which < 2, noise_high, jnp.where(which == 2, noise_low, 0.0))
    picked_from[pl.ds(704, 64), pl.ds(0, WIDTH)] = noise_rows.astype(BF16)
    picked_from[pl.ds(576, 192), pl.ds(WIDTH, WIDTH)] = jnp.zeros((192, WIDTH), BF16)
    hidden = jnp.dot(
        emb_ref[...], time_embed[...], precision=lax.Precision.HIGHEST, preferred_element_type=F32
    )
    hidden = jnp.maximum(hidden, 0.0)

    def layer(l, carry):
        now = lax.rem(l, 2)
        later = 1 - now

        def early(ch, carry):
            at = pl.ds(pl.multiple_of(ch * CHUNK, CHUNK), CHUNK)
            averaged_early[at] = dot(mix[at, pl.ds(0, EARLY)], edges[now, pl.ds(0, EARLY)])
            return carry

        lax.fori_loop(0, ROWS // CHUNK, early, 0)
        nodes = hist[l]
        own = dot(nodes, own_w[l])
        time_row = jnp.dot(
            hidden, time_layer[l], precision=lax.Precision.HIGHEST, preferred_element_type=F32
        )
        high, low = split(own[:, :WIDTH] + time_row[0:1])
        picked_from[pl.ds(576, 64), pl.ds(0, WIDTH)] = high.astype(BF16)
        picked_from[pl.ds(640, 64), pl.ds(0, WIDTH)] = low.astype(BF16)
        picked_from[pl.ds(512, 64)] = dot(nodes, nbr_w[l]).astype(BF16)
        for d in range(8):
            node_copy(l, d, node_ref).wait_recv()
        picked_from[pl.ds(0, 512)] = dot(nodes_in[l], nbr_w[l]).astype(BF16)
        for d in range(8):
            edge_copy(l, d).wait_recv()
        edges[now, pl.ds(ROWS, INCOMING)] = edges_in[l]

        def late(ch, total):
            at = pl.ds(pl.multiple_of(ch * CHUNK, CHUNK), CHUNK)
            averaged = averaged_early[at] + dot(
                mix[at, pl.ds(EARLY, LOOKUP - EARLY)], edges[now, pl.ds(EARLY, LOOKUP - EARLY)]
            )
            averaged = averaged.astype(BF16)
            picked = dot(pick[at], picked_from[...])
            pre = picked[:, :WIDTH] + dot(averaged, edge_w[l])
            message = picked[:, WIDTH:]
            gated = message + jnp.tanh(0.5 * pre) * message
            total = total + jnp.sum(gated.reshape(CHUNK // CITIES, CITIES, WIDTH), axis=0)
            following = averaged.astype(F32) + jnp.maximum(norm(pre), 0.0)
            edges[later, at] = following.astype(BF16)
            return total

        total = lax.fori_loop(0, ROWS // CHUNK, late, jnp.zeros((CITIES, WIDTH), F32))
        update = jnp.maximum(norm(own[:, WIDTH:] + 0.5 * total), 0.0)
        hist[l + 1] = (nodes.astype(F32) + update).astype(BF16)

        @pl.when(l < LAYERS - 1)
        def _():
            edges_sent[l + 1] = dot(send_hot[...], edges[later, pl.ds(0, ROWS)]).astype(BF16)
            for d in range(8):
                node_copy(l + 1, d, hist.at[l + 1]).start()
            for d in range(8):
                edge_copy(l + 1, d).start()

        return carry

    lax.fori_loop(0, LAYERS, layer, 0)
    store = pltpu.make_async_copy(edges.at[LAYERS % 2, pl.ds(0, ROWS)], edge_out, copy_sem)
    store.start()
    node_out[...] = hist[LAYERS]

    def drain(l, carry):
        for d in range(8):
            node_copy(l, d, node_ref).wait_send()
            edge_copy(l, d).wait_send()
        return carry

    lax.fori_loop(0, LAYERS, drain, 0)
    store.wait()


def on_device(
    grid_y,
    grid_x,
    node_state,
    edge_state,
    noisy_edges,
    timestep,
    neighbors,
    mirror_src,
    send_rows,
    node_own,
    node_nbr,
    edge_weight,
    noise_embed,
    time_embed,
    time_layer,
):
    half = WIDTH // 2
    frequency = jnp.exp(-math.log(10000.0) * jnp.arange(half, dtype=F32) / half)
    phases = timestep[0].astype(F32) * frequency
    embedding = jnp.concatenate([jnp.cos(phases), jnp.sin(phases)])[None, :]
    embedding = jnp.broadcast_to(embedding, (8, WIDTH))
    edge_rows = jnp.transpose(edge_state, (1, 0, 2)).reshape(ROWS, WIDTH)
    vmem = pl.BlockSpec(memory_space=pltpu.VMEM)
    hbm = pl.BlockSpec(memory_space=pl.ANY)
    node_out, edge_out = pl.pallas_call(
        functools.partial(kernel, grid_y, grid_x),
        out_shape=(
            jax.ShapeDtypeStruct((CITIES, WIDTH), BF16),
            jax.ShapeDtypeStruct((ROWS, WIDTH), BF16),
        ),
        in_specs=[vmem, hbm] + [vmem] * 11,
        out_specs=(vmem, hbm),
        scratch_shapes=[
            pltpu.VMEM((ROWS, LOOKUP), BF16),
            pltpu.VMEM((ROWS, PICK), BF16),
            pltpu.VMEM((2, LOOKUP, WIDTH), BF16),
            pltpu.VMEM((ROWS, WIDTH), F32),
            pltpu.VMEM((PICK, 2 * WIDTH), BF16),
            pltpu.VMEM((INCOMING, ROWS), BF16),
            pltpu.VMEM((SLOTS, CITIES), F32),
            pltpu.VMEM((LAYERS + 1, CITIES, WIDTH), BF16),
            pltpu.VMEM((LAYERS, 8 * CITIES, WIDTH), BF16),
            pltpu.VMEM((LAYERS, INCOMING, WIDTH), BF16),
            pltpu.VMEM((LAYERS, INCOMING, WIDTH), BF16),
            pltpu.SemaphoreType.DMA((LAYERS, 16)),
            pltpu.SemaphoreType.DMA((LAYERS, 16)),
            pltpu.SemaphoreType.DMA,
        ],
        compiler_params=pltpu.CompilerParams(
            collective_id=0, has_side_effects=True, vmem_limit_bytes=60 * 1024 * 1024
        ),
    )(
        node_state,
        edge_rows,
        noisy_edges.T,
        neighbors.T,
        mirror_src.T,
        send_rows,
        node_own,
        node_nbr,
        edge_weight,
        noise_embed[None, :],
        embedding,
        time_embed,
        time_layer,
    )
    edge_out = edge_out.reshape(SLOTS, CITIES, WIDTH)
    return (node_out, jnp.transpose(edge_out, (1, 0, 2)))


def solution(mesh):
    rows = P(("ty", "tx"), None)
    cubes = P(("ty", "tx"), None, None)
    return jax.shard_map(
        functools.partial(on_device, mesh.shape["ty"], mesh.shape["tx"]),
        mesh=mesh,
        in_specs=(rows, cubes, rows, P(), rows, rows, cubes) + (P(),) * 6,
        out_specs=(rows, cubes),
        check_vma=False,
    )
```

```python
import functools
import math

import jax
import jax.numpy as jnp
from jax import lax
from jax.experimental import pallas as pl
from jax.experimental.pallas import tpu as pltpu
from jax.sharding import PartitionSpec as P

LAYERS = 3
CITIES = 64
SLOTS = 50
WIDTH = 256
HALF = 128
ROWS = CITIES * SLOTS
CAP = 16
INCOMING = 8 * CAP
PICK = 768
CHUNK = 640
CHUNKS = ROWS // CHUNK
GROUP = 2
MESH = pl.DeviceIdType.MESH
F32 = jnp.float32
BF16 = jnp.bfloat16
OFFSETS = [(y, x) for y in (-1, 0, 1) for x in (-1, 0, 1) if (y, x) != (0, 0)]


def norm(values):
    centered = values - jnp.mean(values, axis=-1, keepdims=True)
    spread = jnp.mean(centered * centered, axis=-1, keepdims=True)
    return centered * lax.rsqrt(spread + 1e-05)


def split(values):
    high = values.astype(BF16).astype(F32)
    return high, values - high


def dot(a, b):
    return jnp.dot(a, b, preferred_element_type=F32)


def exact_dot(a, b):
    return jnp.dot(a, b, precision=lax.Precision.HIGHEST, preferred_element_type=F32)


def column(row, eye):
    return jnp.sum(jnp.where(eye, jnp.broadcast_to(row, eye.shape), 0.0), axis=1, keepdims=True)


def halves(ref, start, count):
    left = ref[pl.ds(start * 2, count, stride=2), :]
    right = ref[pl.ds(start * 2 + 1, count, stride=2), :]
    return jnp.concatenate([left, right], axis=1)


def put_halves(ref, start, values):
    count = values.shape[0]
    ref[pl.ds(start * 2, count, stride=2), :] = values[:, :HALF]
    ref[pl.ds(start * 2 + 1, count, stride=2), :] = values[:, HALF:]


def kernel(
    grid_y,
    grid_x,
    node_ref,
    edge_hbm,
    noisy_ref,
    nbr_ref,
    mirror_ref,
    row_at,
    send_at,
    own_hbm,
    nbr_hbm,
    edge_w_hbm,
    noise_ref,
    emb_ref,
    time_embed_hbm,
    time_layer_hbm,
    node_out,
    edge_out,
    own_w,
    nbr_w,
    edge_w,
    time_embed,
    time_layer,
    raw,
    own_0,
    own_1,
    own_2,
    own_3,
    wide_0,
    wide_1,
    wide_2,
    gathered,
    pick,
    reach,
    picked_from,
    pre_buf,
    message_buf,
    averaged_buf,
    fields,
    sent_wide,
    time_rows,
    hist,
    nodes_in,
    edges_in,
    edges_sent,
    send_sem,
    recv_sem,
    copy_sem,
):
    owns = [own_0, own_1, own_2, own_3]
    wides = [wide_0, wide_1, wide_2]
    here_y = lax.axis_index("ty")
    here_x = lax.axis_index("tx")
    targets = [
        (lax.rem(here_y - y + grid_y, grid_y), lax.rem(here_x - x + grid_x, grid_x))
        for y, x in OFFSETS
    ]
    barrier = pltpu.get_barrier_semaphore()
    for target in targets:
        pl.semaphore_signal(barrier, inc=1, device_id=target, device_id_type=MESH)

    pairs = [
        (edge_hbm, raw),
        (time_embed_hbm, time_embed),
        (time_layer_hbm, time_layer),
        (own_hbm, own_w),
        (nbr_hbm, nbr_w),
        (edge_w_hbm, edge_w),
    ]
    loads = [pltpu.make_async_copy(s, t, copy_sem.at[i]) for i, (s, t) in enumerate(pairs)]
    for load in loads:
        load.start()

    def node_copy(layer, d, source):
        return pltpu.make_async_remote_copy(
            src_ref=source,
            dst_ref=nodes_in.at[layer, pl.ds(d * CITIES, CITIES)],
            send_sem=send_sem.at[layer, d],
            recv_sem=recv_sem.at[layer, d],
            device_id=targets[d],
            device_id_type=MESH,
        )

    def edge_copy(layer, d):
        return pltpu.make_async_remote_copy(
            src_ref=edges_sent.at[layer, pl.ds(d * CAP, CAP)],
            dst_ref=edges_in.at[layer, pl.ds(d * CAP, CAP)],
            send_sem=send_sem.at[layer, 8 + d],
            recv_sem=recv_sem.at[layer, 8 + d],
            device_id=targets[d],
            device_id_type=MESH,
        )

    nbr = nbr_ref[...]
    valid = nbr >= 0
    safe = jnp.maximum(nbr, 0)
    tile = safe >> 6
    rel = ((tile >> 4) - here_y + 1) * 3 + (tile & 15) - here_x + 1
    block = jnp.where(rel < 4, rel, jnp.where(rel == 4, 8, rel - 1))
    pick_at = jnp.where(valid, block * CITIES + (safe & 63), -1)
    mirror = mirror_ref[...]
    came = (mirror - ROWS) >> 4
    came = came + jnp.where(came >= 4, 1, 0)
    came_y = (came * 11) >> 5
    from_y = here_y + came_y - 1
    from_x = here_x + (came - 3 * came_y) - 1
    inside = (from_y >= 0) & (from_y < grid_y) & (from_x >= 0) & (from_x < grid_x)
    is_far = mirror >= ROWS
    far_at = jnp.where(valid & is_far & inside, mirror - ROWS, -1)
    fields[...] = ((far_at + 1) + (pick_at + 1) * 256).astype(F32)
    hist[0] = node_ref[...]
    for wide in wides:
        wide[pl.ds(2 * ROWS, 8)] = jnp.zeros((8, HALF), F32)
    noise_high, noise_low = split(noise_ref[...])
    which = lax.broadcasted_iota(jnp.int32, (CITIES, WIDTH), 0)
    noise_rows = jnp.where(which < 2, noise_high, jnp.where(which == 2, noise_low, 0.0))
    picked_from[pl.ds(704, 64), pl.ds(0, WIDTH)] = noise_rows.astype(BF16)
    picked_from[pl.ds(576, 192), pl.ds(WIDTH, WIDTH)] = jnp.zeros((192, WIDTH), BF16)

    loads[0].wait()

    def widen(ch, carry):
        at = pl.multiple_of(ch * CHUNK, CHUNK)
        put_halves(wide_0, at, raw[pl.ds(at, CHUNK)].astype(F32))
        return carry

    lax.fori_loop(0, CHUNKS, widen, 0)

    def send_edges(l):
        for d in range(8):
            for p in range(CAP):
                at = send_at[d, p]
                to = (d * CAP + p) * 2
                sent_wide[pl.ds(to, 1), :] = wides[l][pl.ds(at, 1), :]
                sent_wide[pl.ds(to + 1, 1), :] = wides[l][pl.ds(at + 1, 1), :]
        edges_sent[l] = halves(sent_wide, 0, INCOMING).astype(BF16)
        for d in range(8):
            edge_copy(l, d).start()

    pl.semaphore_wait(barrier, 8)
    for d in range(8):
        node_copy(0, d, node_ref).start()
    send_edges(0)

    def gather_slot(l, k):
        for c in range(CITIES):
            at = row_at[k, c]
            to = (k * CITIES + c) * 2
            gathered[pl.ds(to, 1), :] = wides[l][pl.ds(at, 1), :]
            gathered[pl.ds(to + 1, 1), :] = wides[l][pl.ds(at + 1, 1), :]

    eye = lax.broadcasted_iota(jnp.int32, (CITIES, CITIES), 1)
    eye = eye == lax.broadcasted_iota(jnp.int32, (CITIES, CITIES), 0)
    lanes = lax.broadcasted_iota(jnp.int32, (CITIES, HALF), 1)
    rows = lax.broadcasted_iota(jnp.int32, (CITIES, HALF), 0)
    zero = jnp.zeros((CITIES, HALF), BF16)

    def build(k, carry):
        at = pl.ds(pl.multiple_of(k * CITIES, CITIES), CITIES)
        packed = column(fields[pl.ds(k, 1)], eye).astype(jnp.int32)
        noise = column(noisy_ref[pl.ds(k, 1)], eye)
        packed = jnp.broadcast_to(packed, (CITIES, HALF))
        pick_at = (packed >> 8) - 1
        far_at = (packed & 255) - 1
        live = jnp.where(pick_at >= 0, 1.0, 0.0)
        reach[at] = jnp.where(lanes == far_at, 1.0, 0.0).astype(BF16)
        low = jnp.where(lanes == (pick_at & 127), 1.0, 0.0).astype(BF16)
        high = (pick_at >> 7).astype(F32).astype(BF16)
        hots = [jnp.where(high == jnp.asarray(t, BF16), low, zero) for t in range(5)]
        for t in range(4):
            pick[at, pl.ds(t * HALF, HALF)] = hots[t]
        own = jnp.where(lanes == rows + CITIES, live, 0.0)
        pick[at, pl.ds(512, HALF)] = hots[4] + own.astype(BF16)
        noise_high, noise_low = split(noise * live)
        rest = jnp.where(lanes == rows, live, 0.0)
        rest = jnp.where((lanes == 64) | (lanes == 66), noise_high, rest)
        rest = jnp.where(lanes == 65, noise_low, rest)
        pick[at, pl.ds(640, HALF)] = rest.astype(BF16)
        live = live.astype(BF16)
        own_0[at, pl.ds(0, HALF)] = raw[at, pl.ds(0, HALF)] * live
        own_0[at, pl.ds(HALF, HALF)] = raw[at, pl.ds(HALF, HALF)] * live
        gather_slot(0, k)
        return carry

    lax.fori_loop(0, SLOTS, build, 0)

    for load in loads[1:]:
        load.wait()
    hidden = jnp.maximum(exact_dot(emb_ref[...], time_embed[...]), 0.0)
    for l in range(LAYERS):
        time_rows[pl.ds(8 * l, 8)] = exact_dot(hidden, time_layer[l])

    for l in range(LAYERS):
        if l > 0:

            def gather(g, carry, l=l):
                for step in range(GROUP):
                    gather_slot(l, g * GROUP + step)
                return carry

            lax.fori_loop(0, SLOTS // GROUP, gather, 0)
        nodes = hist[l]
        own = dot(nodes, own_w[l])
        high, low = split(own[:, :WIDTH] + time_rows[pl.ds(8 * l, 1)])
        picked_from[pl.ds(576, 64), pl.ds(0, WIDTH)] = high.astype(BF16)
        picked_from[pl.ds(640, 64), pl.ds(0, WIDTH)] = low.astype(BF16)
        picked_from[pl.ds(512, 64)] = dot(nodes, nbr_w[l]).astype(BF16)
        for d in range(8):
            node_copy(l, d, node_ref).wait_recv()
        picked_from[pl.ds(0, 512)] = dot(nodes_in[l], nbr_w[l]).astype(BF16)
        for d in range(8):
            edge_copy(l, d).wait_recv()

        def multiply(ch, l=l):
            start = pl.multiple_of(ch * CHUNK, CHUNK)
            at = pl.ds(start, CHUNK)
            partner = halves(gathered, start, CHUNK) + dot(reach[at], edges_in[l])
            averaged = ((owns[l][at].astype(F32) + partner) * 0.5).astype(BF16)
            picked = dot(pick[at], picked_from[...])
            averaged_buf[...] = averaged
            pre_buf[...] = picked[:, :WIDTH] + dot(averaged, edge_w[l])
            message_buf[...] = picked[:, WIDTH:].astype(BF16)

        def apply(ch, total, l=l):
            start = pl.multiple_of(ch * CHUNK, CHUNK)
            pre = pre_buf[...]
            message = message_buf[...].astype(F32)
            gated = message + jnp.tanh(0.5 * pre) * message
            total = total + jnp.sum(gated.reshape(CHUNK // CITIES, CITIES, WIDTH), axis=0)
            following = averaged_buf[...].astype(F32) + jnp.maximum(norm(pre), 0.0)
            following = following.astype(BF16)
            owns[l + 1][pl.ds(start, CHUNK)] = following
            if l + 1 < LAYERS:
                put_halves(wides[l + 1], start, following.astype(F32))
            return total

        def both(ch, total):
            total = apply(ch - 1, total)
            multiply(ch)
            return total

        multiply(0)
        total = lax.fori_loop(1, CHUNKS, both, jnp.zeros((CITIES, WIDTH), F32))
        total = apply(CHUNKS - 1, total)
        update = jnp.maximum(norm(own[:, WIDTH:] + 0.5 * total), 0.0)
        hist[l + 1] = (nodes.astype(F32) + update).astype(BF16)
        if l + 1 < LAYERS:
            send_edges(l + 1)
            for d in range(8):
                node_copy(l + 1, d, hist.at[l + 1]).start()

    store = pltpu.make_async_copy(own_3, edge_out, copy_sem.at[0])
    store.start()
    node_out[...] = hist[LAYERS]

    def drain(l, carry):
        for d in range(8):
            node_copy(l, d, node_ref).wait_send()
            edge_copy(l, d).wait_send()
        return carry

    lax.fori_loop(0, LAYERS, drain, 0)
    store.wait()


def by_slot(row):
    city = row // SLOTS
    return (row - city * SLOTS) * CITIES + city


def on_device(
    grid_y,
    grid_x,
    node_state,
    edge_state,
    noisy_edges,
    timestep,
    neighbors,
    mirror_src,
    send_rows,
    node_own,
    node_nbr,
    edge_weight,
    noise_embed,
    time_embed,
    time_layer,
):
    half = WIDTH // 2
    frequency = jnp.exp(-math.log(10000.0) * jnp.arange(half, dtype=F32) / half)
    phases = timestep[0].astype(F32) * frequency
    embedding = jnp.concatenate([jnp.cos(phases), jnp.sin(phases)])[None, :]
    embedding = jnp.broadcast_to(embedding, (8, WIDTH))
    edge_rows = jnp.transpose(edge_state, (1, 0, 2)).reshape(ROWS, WIDTH)
    vmem = pl.BlockSpec(memory_space=pltpu.VMEM)
    hbm = pl.BlockSpec(memory_space=pl.ANY)
    smem = pl.BlockSpec(memory_space=pltpu.SMEM)
    nbr, mirror = neighbors.T, mirror_src.T
    itself = jnp.arange(ROWS, dtype=jnp.int32).reshape(SLOTS, CITIES)
    partner_at = jnp.where(mirror >= 0, jnp.where(mirror >= ROWS, ROWS, by_slot(mirror)), itself)
    row_at = jnp.where(nbr >= 0, partner_at, ROWS) * 2
    send_at = jnp.where(send_rows[0] >= 0, by_slot(send_rows[0]), ROWS) * 2
    node_out, edge_out = pl.pallas_call(
        functools.partial(kernel, grid_y, grid_x),
        out_shape=(
            jax.ShapeDtypeStruct((CITIES, WIDTH), BF16),
            jax.ShapeDtypeStruct((ROWS, WIDTH), BF16),
        ),
        in_specs=[vmem, hbm] + [vmem] * 3 + [smem] * 2 + [hbm] * 3 + [vmem] * 2 + [hbm] * 2,
        out_specs=(vmem, hbm),
        scratch_shapes=[
            pltpu.VMEM((LAYERS, WIDTH, 2 * WIDTH), BF16),
            pltpu.VMEM((LAYERS, WIDTH, 2 * WIDTH), BF16),
            pltpu.VMEM((LAYERS, WIDTH, WIDTH), BF16),
            pltpu.VMEM((WIDTH, WIDTH), F32),
            pltpu.VMEM((LAYERS, WIDTH, WIDTH), F32),
            pltpu.VMEM((ROWS, WIDTH), BF16),
        ]
        + [pltpu.VMEM((ROWS, WIDTH), BF16)] * 4
        + [pltpu.VMEM((2 * ROWS + 8, HALF), F32)] * 3
        + [
            pltpu.VMEM((2 * ROWS, HALF), F32),
            pltpu.VMEM((ROWS, PICK), BF16),
            pltpu.VMEM((ROWS, INCOMING), BF16),
            pltpu.VMEM((PICK, 2 * WIDTH), BF16),
            pltpu.VMEM((CHUNK, WIDTH), F32),
            pltpu.VMEM((CHUNK, WIDTH), BF16),
            pltpu.VMEM((CHUNK, WIDTH), BF16),
            pltpu.VMEM((SLOTS, CITIES), F32),
            pltpu.VMEM((2 * INCOMING, HALF), F32),
            pltpu.VMEM((8 * LAYERS, WIDTH), F32),
            pltpu.VMEM((LAYERS + 1, CITIES, WIDTH), BF16),
            pltpu.VMEM((LAYERS, 8 * CITIES, WIDTH), BF16),
            pltpu.VMEM((LAYERS, INCOMING, WIDTH), BF16),
            pltpu.VMEM((LAYERS, INCOMING, WIDTH), BF16),
            pltpu.SemaphoreType.DMA((LAYERS, 16)),
            pltpu.SemaphoreType.DMA((LAYERS, 16)),
            pltpu.SemaphoreType.DMA((8,)),
        ],
        compiler_params=pltpu.CompilerParams(
            collective_id=0, has_side_effects=True, vmem_limit_bytes=44 * 1024 * 1024
        ),
    )(
        node_state,
        edge_rows,
        noisy_edges.T,
        nbr,
        mirror,
        row_at,
        send_at,
        node_own,
        node_nbr,
        edge_weight,
        noise_embed[None, :],
        embedding,
        time_embed,
        time_layer,
    )
    edge_out = edge_out.reshape(SLOTS, CITIES, WIDTH)
    return (node_out, jnp.transpose(edge_out, (1, 0, 2)))


def solution(mesh):
    rows = P(("ty", "tx"), None)
    cubes = P(("ty", "tx"), None, None)
    return jax.shard_map(
        functools.partial(on_device, mesh.shape["ty"], mesh.shape["tx"]),
        mesh=mesh,
        in_specs=(rows, cubes, rows, P(), rows, rows, cubes) + (P(),) * 6,
        out_specs=(rows, cubes),
        check_vma=False,
    )
```

```python
import functools
import math

import jax
import jax.numpy as jnp
from jax import lax
from jax.experimental import pallas as pl
from jax.experimental.pallas import tpu as pltpu
from jax.sharding import PartitionSpec as P

LAYERS = 3
CITIES = 64
SLOTS = 50
WIDTH = 256
HALF = 128
ROWS = CITIES * SLOTS
CAP = 16
INCOMING = 8 * CAP
PICK = 768
CHUNK = 640
CHUNKS = ROWS // CHUNK
GROUP = 2
AHEAD = 2
LATE = 1600
MESH = pl.DeviceIdType.MESH
F32 = jnp.float32
BF16 = jnp.bfloat16
OFFSETS = [(y, x) for y in (-1, 0, 1) for x in (-1, 0, 1) if (y, x) != (0, 0)]


def norm(values, epsilon=1e-05):
    centered = values - jnp.mean(values, axis=-1, keepdims=True)
    spread = jnp.mean(centered * centered, axis=-1, keepdims=True)
    return centered * lax.rsqrt(spread + epsilon)


def split(values):
    high = values.astype(BF16).astype(F32)
    return high, values - high


def dot(a, b):
    return jnp.dot(a, b, preferred_element_type=F32)


def exact_dot(a, b):
    return jnp.dot(a, b, precision=lax.Precision.HIGHEST, preferred_element_type=F32)


def column(row, eye):
    return jnp.sum(jnp.where(eye, jnp.broadcast_to(row, eye.shape), 0.0), axis=1, keepdims=True)


def halves(ref, start, count):
    left = ref[pl.ds(start * 2, count, stride=2), :]
    right = ref[pl.ds(start * 2 + 1, count, stride=2), :]
    return jnp.concatenate([left, right], axis=1)


def put_halves(ref, start, values):
    count = values.shape[0]
    ref[pl.ds(start * 2, count, stride=2), :] = values[:, :HALF]
    ref[pl.ds(start * 2 + 1, count, stride=2), :] = values[:, HALF:]


def kernel(
    grid_y,
    grid_x,
    node_hbm,
    edge_hbm,
    noisy_hbm,
    nbr_ids_hbm,
    mirror_hbm,
    row_at,
    send_at,
    own_hbm,
    nbr_hbm,
    edge_w_hbm,
    noise_hbm,
    emb_ref,
    time_embed_hbm,
    time_layer_hbm,
    node_out,
    edge_out,
    node_ref,
    noisy_ref,
    nbr_ref,
    mirror_ref,
    noise_ref,
    own_w,
    nbr_w,
    edge_w,
    time_embed,
    time_layer,
    raw,
    own_0,
    own_3,
    wide_0,
    wide_1,
    wide_2,
    gathered,
    pick,
    reach,
    picked_from,
    pre_part,
    messages,
    fields,
    sent_wide,
    time_rows,
    hist,
    nodes_in,
    edges_in,
    edges_sent,
    send_sem,
    recv_sem,
    copy_sem,
):
    wides = [wide_0, wide_1, wide_2]
    here_y = lax.axis_index("ty")
    here_x = lax.axis_index("tx")
    targets = [
        (lax.rem(here_y - y + grid_y, grid_y), lax.rem(here_x - x + grid_x, grid_x))
        for y, x in OFFSETS
    ]
    barrier = pltpu.get_barrier_semaphore()
    for target in targets:
        pl.semaphore_signal(barrier, inc=1, device_id=target, device_id_type=MESH)

    pairs = [
        (nbr_ids_hbm, nbr_ref),
        (mirror_hbm, mirror_ref),
        (noise_hbm, noise_ref),
        (node_hbm, node_ref),
        (noisy_hbm, noisy_ref),
        (edge_hbm, raw),
        (time_embed_hbm, time_embed),
        (time_layer_hbm, time_layer),
        (own_hbm, own_w),
        (nbr_hbm, nbr_w),
        (edge_w_hbm, edge_w),
    ]
    loads = [pltpu.make_async_copy(s, t, copy_sem.at[i]) for i, (s, t) in enumerate(pairs)]
    for load in loads:
        load.start()
    for load in loads[:5]:
        load.wait()

    def node_copy(layer, d, source):
        return pltpu.make_async_remote_copy(
            src_ref=source,
            dst_ref=nodes_in.at[layer, pl.ds(d * CITIES, CITIES)],
            send_sem=send_sem.at[layer, d],
            recv_sem=recv_sem.at[layer, d],
            device_id=targets[d],
            device_id_type=MESH,
        )

    def edge_copy(layer, d):
        return pltpu.make_async_remote_copy(
            src_ref=edges_sent.at[layer, pl.ds(d * CAP, CAP)],
            dst_ref=edges_in.at[layer, pl.ds(d * CAP, CAP)],
            send_sem=send_sem.at[layer, 8 + d],
            recv_sem=recv_sem.at[layer, 8 + d],
            device_id=targets[d],
            device_id_type=MESH,
        )

    nbr = nbr_ref[...]
    valid = nbr >= 0
    safe = jnp.maximum(nbr, 0)
    tile = safe >> 6
    rel = ((tile >> 4) - here_y + 1) * 3 + (tile & 15) - here_x + 1
    block = jnp.where(rel < 4, rel, jnp.where(rel == 4, 8, rel - 1))
    pick_at = jnp.where(valid, block * CITIES + (safe & 63), -1)
    mirror = mirror_ref[...]
    came = (mirror - ROWS) >> 4
    came = came + jnp.where(came >= 4, 1, 0)
    came_y = (came * 11) >> 5
    from_y = here_y + came_y - 1
    from_x = here_x + (came - 3 * came_y) - 1
    inside = (from_y >= 0) & (from_y < grid_y) & (from_x >= 0) & (from_x < grid_x)
    is_far = mirror >= ROWS
    far_at = jnp.where(valid & is_far & inside, mirror - ROWS, -1)
    fields[...] = ((far_at + 1) + (pick_at + 1) * 256).astype(F32)
    hist[0] = node_ref[...]
    for wide in wides:
        wide[pl.ds(2 * ROWS, 8)] = jnp.zeros((8, HALF), F32)
    noise_high, noise_low = split(0.5 * noise_ref[...])
    which = lax.broadcasted_iota(jnp.int32, (CITIES, WIDTH), 0)
    noise_rows = jnp.where(which < 2, noise_high, jnp.where(which == 2, noise_low, 0.0))
    picked_from[pl.ds(704, 64), pl.ds(0, WIDTH)] = noise_rows.astype(BF16)
    picked_from[pl.ds(576, 192), pl.ds(WIDTH, WIDTH)] = jnp.zeros((192, WIDTH), BF16)

    loads[5].wait()

    def widen(ch, carry):
        at = pl.multiple_of(ch * CHUNK, CHUNK)
        put_halves(wide_0, at, raw[pl.ds(at, CHUNK)].astype(F32))
        return carry

    lax.fori_loop(0, CHUNKS, widen, 0)

    def send_exchange(l):
        for d in range(8):
            for p in range(CAP):
                at = send_at[d, p]
                to = (d * CAP + p) * 2
                sent_wide[pl.ds(to, 1), :] = wides[l][pl.ds(at, 1), :]
                sent_wide[pl.ds(to + 1, 1), :] = wides[l][pl.ds(at + 1, 1), :]
        for d in range(8):
            node_copy(l, d, hist.at[l] if l else node_ref).start()
        edges_sent[l] = halves(sent_wide, 0, INCOMING).astype(BF16)
        for d in range(8):
            edge_copy(l, d).start()

    loads[6].wait()
    loads[7].wait()
    hidden = jnp.maximum(exact_dot(emb_ref[...], time_embed[...]), 0.0)
    for l in range(LAYERS):
        time_rows[pl.ds(8 * l, 8)] = exact_dot(hidden, time_layer[l])

    pl.semaphore_wait(barrier, 8)
    send_exchange(0)

    def gather_slot(l, k):
        for c in range(CITIES):
            at = row_at[k, c]
            to = (k * CITIES + c) * 2
            gathered[pl.ds(to, 1), :] = wides[l][pl.ds(at, 1), :]
            gathered[pl.ds(to + 1, 1), :] = wides[l][pl.ds(at + 1, 1), :]

    eye = lax.broadcasted_iota(jnp.int32, (CITIES, CITIES), 1)
    eye = eye == lax.broadcasted_iota(jnp.int32, (CITIES, CITIES), 0)
    lanes = lax.broadcasted_iota(jnp.int32, (CITIES, HALF), 1)
    rows = lax.broadcasted_iota(jnp.int32, (CITIES, HALF), 0)
    zero = jnp.zeros((CITIES, HALF), BF16)

    def build_slot(k, packed, noise):
        at = pl.ds(pl.multiple_of(k * CITIES, CITIES), CITIES)
        packed = jnp.broadcast_to(packed.astype(jnp.int32), (CITIES, HALF))
        pick_at = (packed >> 8) - 1
        far_at = (packed & 255) - 1
        live = jnp.where(pick_at >= 0, 1.0, 0.0)
        reach[at] = jnp.where(lanes == far_at, 1.0, 0.0).astype(BF16)
        low = jnp.where(lanes == (pick_at & 127), 1.0, 0.0).astype(BF16)
        high = (pick_at >> 7).astype(F32).astype(BF16)
        hots = [jnp.where(high == jnp.asarray(t, BF16), low, zero) for t in range(5)]
        for t in range(4):
            pick[at, pl.ds(t * HALF, HALF)] = hots[t]
        own = jnp.where(lanes == rows + CITIES, live, 0.0)
        pick[at, pl.ds(512, HALF)] = hots[4] + own.astype(BF16)
        noise_high, noise_low = split(noise * live)
        rest = jnp.where(lanes == rows, live, 0.0)
        rest = jnp.where((lanes == 64) | (lanes == 66), noise_high, rest)
        rest = jnp.where(lanes == 65, noise_low, rest)
        pick[at, pl.ds(640, HALF)] = rest.astype(BF16)
        live = live.astype(BF16)
        own_0[at, pl.ds(0, HALF)] = raw[at, pl.ds(0, HALF)] * live
        own_0[at, pl.ds(HALF, HALF)] = raw[at, pl.ds(HALF, HALF)] * live

    def build(g, carry):
        slots = [g * GROUP + step for step in range(GROUP)]
        found = [(column(fields[pl.ds(k, 1)], eye), column(noisy_ref[pl.ds(k, 1)], eye)) for k in slots]
        for k, (packed, noise) in zip(slots, found):
            build_slot(k, packed, noise)
        for k in slots:
            gather_slot(0, k)
        return carry

    lax.fori_loop(0, SLOTS // GROUP, build, 0)

    for load in loads[8:]:
        load.wait()
    for l in range(LAYERS):
        edge_w[l] = edge_w[l] * jnp.asarray(0.25 / 2**l, BF16)

    def project(nodes, l):
        values = dot(nodes, nbr_w[l])
        return jnp.concatenate([values[:, :WIDTH] * 0.5, values[:, WIDTH:]], axis=1).astype(BF16)

    for l in range(LAYERS):
        ahead = CHUNKS if l == 0 else AHEAD

        def gather(g, carry, l=l):
            for step in range(GROUP):
                gather_slot(l, g * GROUP + step)
            return carry

        def pick_chunk(ch):
            at = pl.ds(pl.multiple_of(ch * CHUNK, CHUNK), CHUNK)
            picked = dot(pick[at], picked_from[...])
            pre_part[at] = picked[:, :WIDTH]
            messages[at] = picked[:, WIDTH:]

        def gather_and_pick(ch, carry, l=l):
            pick_chunk(ch)
            for step in range(CHUNK // CITIES):
                gather_slot(l, (ch + AHEAD) * (CHUNK // CITIES) + step)
            return carry

        def pick_only(ch, carry):
            pick_chunk(ch)
            return carry

        nodes = hist[l]
        own = dot(nodes, own_w[l])
        high, low = split(0.5 * (own[:, :WIDTH] + time_rows[pl.ds(8 * l, 1)]))
        picked_from[pl.ds(576, 64), pl.ds(0, WIDTH)] = high.astype(BF16)
        picked_from[pl.ds(640, 64), pl.ds(0, WIDTH)] = low.astype(BF16)
        picked_from[pl.ds(512, 64)] = project(nodes, l)
        if l > 0:
            lax.fori_loop(0, AHEAD * CHUNK // CITIES // GROUP, gather, 0)
        for d in range(8):
            node_copy(l, d, node_ref).wait_recv()
        picked_from[pl.ds(0, 512)] = project(nodes_in[l], l)
        lax.fori_loop(0, CHUNKS - ahead, gather_and_pick, 0)
        lax.fori_loop(CHUNKS - ahead, CHUNKS, pick_only, 0)
        for d in range(8):
            edge_copy(l, d).wait_recv()

        def late(ch, total, l=l):
            start = pl.multiple_of(ch * LATE, LATE)
            at = pl.ds(start, LATE)
            mine = own_0[at].astype(F32) if l == 0 else halves(wides[l], start, LATE)
            both = mine + halves(gathered, start, LATE) + dot(reach[at], edges_in[l])
            pre = pre_part[at] + dot(both.astype(BF16), edge_w[l])
            message = messages[at]
            gated = message + jnp.tanh(pre) * message
            total = total + jnp.sum(gated.reshape(LATE // CITIES, CITIES, WIDTH), axis=0)
            centered = pre - jnp.mean(pre, axis=-1, keepdims=True)
            spread = jnp.sum(centered * centered, axis=-1, keepdims=True)
            scale = lax.rsqrt(spread + 0.25e-05 * WIDTH) * (WIDTH**0.5 * 2 ** (l + 1))
            following = both + jnp.maximum(centered * scale, 0.0)
            if l + 1 < LAYERS:
                put_halves(wides[l + 1], start, following)
            else:
                own_3[at] = (following * 0.5 ** (l + 1)).astype(BF16)
            return total

        total = lax.fori_loop(0, ROWS // LATE, late, jnp.zeros((CITIES, WIDTH), F32))
        update = jnp.maximum(norm(own[:, WIDTH:] + 0.5 * total), 0.0)
        hist[l + 1] = (nodes.astype(F32) + update).astype(BF16)
        if l + 1 < LAYERS:
            send_exchange(l + 1)

    store = pltpu.make_async_copy(own_3, edge_out, copy_sem.at[0])
    store.start()
    node_out[...] = hist[LAYERS]

    def drain(l, carry):
        for d in range(8):
            node_copy(l, d, node_ref).wait_send()
            edge_copy(l, d).wait_send()
        return carry

    lax.fori_loop(0, LAYERS, drain, 0)
    store.wait()


def by_slot(row):
    city = row // SLOTS
    return (row - city * SLOTS) * CITIES + city


def in_hbm(array):
    return pltpu.with_memory_space_constraint(array, pltpu.HBM)


def on_device(
    grid_y,
    grid_x,
    node_state,
    edge_state,
    noisy_edges,
    timestep,
    neighbors,
    mirror_src,
    send_rows,
    node_own,
    node_nbr,
    edge_weight,
    noise_embed,
    time_embed,
    time_layer,
):
    half = WIDTH // 2
    frequency = jnp.exp(-math.log(10000.0) * jnp.arange(half, dtype=F32) / half)
    phases = timestep[0].astype(F32) * frequency
    embedding = jnp.concatenate([jnp.cos(phases), jnp.sin(phases)])[None, :]
    embedding = jnp.broadcast_to(embedding, (8, WIDTH))
    edge_rows = jnp.transpose(edge_state, (1, 0, 2)).reshape(ROWS, WIDTH)
    vmem = pl.BlockSpec(memory_space=pltpu.VMEM)
    hbm = pl.BlockSpec(memory_space=pltpu.HBM)
    smem = pl.BlockSpec(memory_space=pltpu.SMEM)
    nbr, mirror = neighbors.T, mirror_src.T
    itself = jnp.arange(ROWS, dtype=jnp.int32).reshape(SLOTS, CITIES)
    partner_at = jnp.where(mirror >= 0, jnp.where(mirror >= ROWS, ROWS, by_slot(mirror)), itself)
    row_at = jnp.where(nbr >= 0, partner_at, ROWS) * 2
    send_at = jnp.where(send_rows[0] >= 0, by_slot(send_rows[0]), ROWS) * 2
    node_out, edge_out = pl.pallas_call(
        functools.partial(kernel, grid_y, grid_x),
        out_shape=(
            jax.ShapeDtypeStruct((CITIES, WIDTH), BF16),
            jax.ShapeDtypeStruct((ROWS, WIDTH), BF16),
        ),
        in_specs=[hbm] * 5 + [smem] * 2 + [hbm] * 4 + [vmem] + [hbm] * 2,
        out_specs=(vmem, pl.BlockSpec(memory_space=pl.ANY)),
        scratch_shapes=[
            pltpu.VMEM((CITIES, WIDTH), BF16),
            pltpu.VMEM((SLOTS, CITIES), F32),
            pltpu.VMEM((SLOTS, CITIES), jnp.int32),
            pltpu.VMEM((SLOTS, CITIES), jnp.int32),
            pltpu.VMEM((1, WIDTH), F32),
            pltpu.VMEM((LAYERS, WIDTH, 2 * WIDTH), BF16),
            pltpu.VMEM((LAYERS, WIDTH, 2 * WIDTH), BF16),
            pltpu.VMEM((LAYERS, WIDTH, WIDTH), BF16),
            pltpu.VMEM((WIDTH, WIDTH), F32),
            pltpu.VMEM((LAYERS, WIDTH, WIDTH), F32),
            pltpu.VMEM((ROWS, WIDTH), BF16),
        ]
        + [pltpu.VMEM((ROWS, WIDTH), BF16)] * 2
        + [pltpu.VMEM((2 * ROWS + 8, HALF), F32)] * 3
        + [
            pltpu.VMEM((2 * ROWS, HALF), F32),
            pltpu.VMEM((ROWS, PICK), BF16),
            pltpu.VMEM((ROWS, INCOMING), BF16),
            pltpu.VMEM((PICK, 2 * WIDTH), BF16),
            pltpu.VMEM((ROWS, WIDTH), F32),
            pltpu.VMEM((ROWS, WIDTH), F32),
            pltpu.VMEM((SLOTS, CITIES), F32),
            pltpu.VMEM((2 * INCOMING, HALF), F32),
            pltpu.VMEM((8 * LAYERS, WIDTH), F32),
            pltpu.VMEM((LAYERS + 1, CITIES, WIDTH), BF16),
            pltpu.VMEM((LAYERS, 8 * CITIES, WIDTH), BF16),
            pltpu.VMEM((LAYERS, INCOMING, WIDTH), BF16),
            pltpu.VMEM((LAYERS, INCOMING, WIDTH), BF16),
            pltpu.SemaphoreType.DMA((LAYERS, 16)),
            pltpu.SemaphoreType.DMA((LAYERS, 16)),
            pltpu.SemaphoreType.DMA((11,)),
        ],
        compiler_params=pltpu.CompilerParams(
            collective_id=0, has_side_effects=True, vmem_limit_bytes=48 * 1024 * 1024
        ),
    )(
        *map(
            in_hbm,
            (
                node_state,
                edge_rows,
                noisy_edges.T,
                nbr,
                mirror,
            ),
        ),
        row_at,
        send_at,
        *map(in_hbm, (node_own, node_nbr, edge_weight, noise_embed[None, :])),
        embedding,
        in_hbm(time_embed),
        in_hbm(time_layer),
    )
    edge_out = edge_out.reshape(SLOTS, CITIES, WIDTH)
    return (node_out, jnp.transpose(edge_out, (1, 0, 2)))


def solution(mesh):
    rows = P(("ty", "tx"), None)
    cubes = P(("ty", "tx"), None, None)
    return jax.shard_map(
        functools.partial(on_device, mesh.shape["ty"], mesh.shape["tx"]),
        mesh=mesh,
        in_specs=(rows, cubes, rows, P(), rows, rows, cubes) + (P(),) * 6,
        out_specs=(rows, cubes),
        check_vma=False,
    )
```

```python
import functools
import math

import jax
import jax.numpy as jnp
from jax import lax
from jax.experimental import pallas as pl
from jax.experimental.pallas import tpu as pltpu
from jax.sharding import PartitionSpec as P

LAYERS = 3
CITIES = 64
SLOTS = 50
WIDTH = 256
HALF = 128
ROWS = CITIES * SLOTS
CAP = 16
INCOMING = 8 * CAP
PICK = 768
CHUNK = 640
CHUNKS = ROWS // CHUNK
GROUP = 2
FAR = 512
MESH = pl.DeviceIdType.MESH
F32 = jnp.float32
BF16 = jnp.bfloat16
OFFSETS = [(y, x) for y in (-1, 0, 1) for x in (-1, 0, 1) if (y, x) != (0, 0)]


def norm(values, epsilon=1e-05):
    centered = values - jnp.mean(values, axis=-1, keepdims=True)
    spread = jnp.mean(centered * centered, axis=-1, keepdims=True)
    return centered * lax.rsqrt(spread + epsilon)


def split(values):
    high = values.astype(BF16).astype(F32)
    return high, values - high


def dot(a, b):
    return jnp.dot(a, b, preferred_element_type=F32)


def exact_dot(a, b):
    return jnp.dot(a, b, precision=lax.Precision.HIGHEST, preferred_element_type=F32)


def column(row, eye):
    return jnp.sum(jnp.where(eye, jnp.broadcast_to(row, eye.shape), 0.0), axis=1, keepdims=True)


def halves(ref, start, count):
    left = ref[pl.ds(start * 2, count, stride=2), :]
    right = ref[pl.ds(start * 2 + 1, count, stride=2), :]
    return jnp.concatenate([left, right], axis=1)


def put_halves(ref, start, values):
    count = values.shape[0]
    ref[pl.ds(start * 2, count, stride=2), :] = values[:, :HALF]
    ref[pl.ds(start * 2 + 1, count, stride=2), :] = values[:, HALF:]


def kernel(
    grid_y,
    grid_x,
    node_hbm,
    edge_hbm,
    noisy_hbm,
    nbr_ids_hbm,
    mirror_hbm,
    row_at,
    send_at,
    own_hbm,
    nbr_hbm,
    edge_w_hbm,
    noise_hbm,
    emb_ref,
    time_embed_hbm,
    time_layer_hbm,
    node_out,
    edge_out,
    node_ref,
    noisy_ref,
    nbr_ref,
    mirror_ref,
    noise_ref,
    own_w,
    nbr_w,
    edge_w,
    time_embed,
    time_layer,
    raw,
    own_0,
    own_3,
    wide_0,
    wide_1,
    wide_2,
    gathered,
    pick,
    reach,
    picked_from,
    pre_part,
    messages,
    pre_buf,
    message_buf,
    both_buf,
    fields,
    sent_wide,
    time_rows,
    hist,
    nodes_in,
    edges_in,
    edges_sent,
    send_sem,
    recv_sem,
    copy_sem,
):
    wides = [wide_0, wide_1, wide_2]
    here_y = lax.axis_index("ty")
    here_x = lax.axis_index("tx")
    targets = [
        (lax.rem(here_y - y + grid_y, grid_y), lax.rem(here_x - x + grid_x, grid_x))
        for y, x in OFFSETS
    ]
    barrier = pltpu.get_barrier_semaphore()
    for target in targets:
        pl.semaphore_signal(barrier, inc=1, device_id=target, device_id_type=MESH)

    pairs = [
        (nbr_ids_hbm, nbr_ref),
        (mirror_hbm, mirror_ref),
        (noise_hbm, noise_ref),
        (node_hbm, node_ref),
        (noisy_hbm, noisy_ref),
        (edge_hbm, raw),
        (time_embed_hbm, time_embed),
        (time_layer_hbm, time_layer),
        (own_hbm, own_w),
        (nbr_hbm, nbr_w),
        (edge_w_hbm, edge_w),
    ]
    loads = [pltpu.make_async_copy(s, t, copy_sem.at[i]) for i, (s, t) in enumerate(pairs)]
    for load in loads:
        load.start()
    for load in loads[:5]:
        load.wait()

    def node_copy(layer, d, source):
        return pltpu.make_async_remote_copy(
            src_ref=source,
            dst_ref=nodes_in.at[layer, pl.ds(d * CITIES, CITIES)],
            send_sem=send_sem.at[layer, d],
            recv_sem=recv_sem.at[layer, d],
            device_id=targets[d],
            device_id_type=MESH,
        )

    def edge_copy(layer, d):
        return pltpu.make_async_remote_copy(
            src_ref=edges_sent.at[layer, pl.ds(d * CAP, CAP)],
            dst_ref=edges_in.at[layer, pl.ds(d * CAP, CAP)],
            send_sem=send_sem.at[layer, 8 + d],
            recv_sem=recv_sem.at[layer, 8 + d],
            device_id=targets[d],
            device_id_type=MESH,
        )

    nbr = nbr_ref[...]
    valid = nbr >= 0
    safe = jnp.maximum(nbr, 0)
    tile = safe >> 6
    rel = ((tile >> 4) - here_y + 1) * 3 + (tile & 15) - here_x + 1
    block = jnp.where(rel < 4, rel, jnp.where(rel == 4, 8, rel - 1))
    pick_at = jnp.where(valid, block * CITIES + (safe & 63), -1)
    mirror = mirror_ref[...]
    came = (mirror - ROWS) >> 4
    came = came + jnp.where(came >= 4, 1, 0)
    came_y = (came * 11) >> 5
    from_y = here_y + came_y - 1
    from_x = here_x + (came - 3 * came_y) - 1
    inside = (from_y >= 0) & (from_y < grid_y) & (from_x >= 0) & (from_x < grid_x)
    is_far = mirror >= ROWS
    far_at = jnp.where(valid & is_far & inside, mirror - ROWS, -1)
    fields[...] = ((far_at + 1) + (pick_at + 1) * 256).astype(F32)
    hist[0] = node_ref[...]
    for wide in wides:
        wide[pl.ds(2 * ROWS, 8)] = jnp.zeros((8, HALF), F32)
    noise_high, noise_low = split(0.5 * noise_ref[...])
    which = lax.broadcasted_iota(jnp.int32, (CITIES, WIDTH), 0)
    noise_rows = jnp.where(which < 2, noise_high, jnp.where(which == 2, noise_low, 0.0))
    picked_from[pl.ds(704, 64), pl.ds(0, WIDTH)] = noise_rows.astype(BF16)
    picked_from[pl.ds(576, 192), pl.ds(WIDTH, WIDTH)] = jnp.zeros((192, WIDTH), BF16)

    loads[5].wait()

    def widen(ch, carry):
        at = pl.multiple_of(ch * CHUNK, CHUNK)
        put_halves(wide_0, at, raw[pl.ds(at, CHUNK)].astype(F32))
        return carry

    lax.fori_loop(0, CHUNKS, widen, 0)

    def send_exchange(l):
        for d in range(8):
            for p in range(CAP):
                at = send_at[d, p]
                to = (d * CAP + p) * 2
                sent_wide[pl.ds(to, 1), :] = wides[l][pl.ds(at, 1), :]
                sent_wide[pl.ds(to + 1, 1), :] = wides[l][pl.ds(at + 1, 1), :]
        for d in range(8):
            node_copy(l, d, hist.at[l] if l else node_ref).start()
        edges_sent[l] = halves(sent_wide, 0, INCOMING).astype(BF16)
        for d in range(8):
            edge_copy(l, d).start()

    loads[6].wait()
    loads[7].wait()
    hidden = jnp.maximum(exact_dot(emb_ref[...], time_embed[...]), 0.0)
    for l in range(LAYERS):
        time_rows[pl.ds(8 * l, 8)] = exact_dot(hidden, time_layer[l])

    pl.semaphore_wait(barrier, 8)
    send_exchange(0)

    def gather_slot(l, k):
        for c in range(CITIES):
            at = row_at[k, c]
            to = (k * CITIES + c) * 2
            gathered[pl.ds(to, 1), :] = wides[l][pl.ds(at, 1), :]
            gathered[pl.ds(to + 1, 1), :] = wides[l][pl.ds(at + 1, 1), :]

    eye = lax.broadcasted_iota(jnp.int32, (CITIES, CITIES), 1)
    eye = eye == lax.broadcasted_iota(jnp.int32, (CITIES, CITIES), 0)
    lanes = lax.broadcasted_iota(jnp.int32, (CITIES, HALF), 1)
    rows = lax.broadcasted_iota(jnp.int32, (CITIES, HALF), 0)
    zero = jnp.zeros((CITIES, HALF), BF16)

    def build_slot(k, packed, noise):
        at = pl.ds(pl.multiple_of(k * CITIES, CITIES), CITIES)
        packed = jnp.broadcast_to(packed.astype(jnp.int32), (CITIES, HALF))
        pick_at = (packed >> 8) - 1
        far_at = (packed & 255) - 1
        live = jnp.where(pick_at >= 0, 1.0, 0.0)
        reach[at] = jnp.where(lanes == far_at, 1.0, 0.0).astype(BF16)
        low = jnp.where(lanes == (pick_at & 127), 1.0, 0.0).astype(BF16)
        high = (pick_at >> 7).astype(F32).astype(BF16)
        hots = [jnp.where(high == jnp.asarray(t, BF16), low, zero) for t in range(5)]
        for t in range(4):
            pick[at, pl.ds(t * HALF, HALF)] = hots[t]
        own = jnp.where(lanes == rows + CITIES, live, 0.0)
        pick[at, pl.ds(512, HALF)] = hots[4] + own.astype(BF16)
        noise_high, noise_low = split(noise * live)
        rest = jnp.where(lanes == rows, live, 0.0)
        rest = jnp.where((lanes == 64) | (lanes == 66), noise_high, rest)
        rest = jnp.where(lanes == 65, noise_low, rest)
        pick[at, pl.ds(640, HALF)] = rest.astype(BF16)
        live = live.astype(BF16)
        own_0[at, pl.ds(0, HALF)] = raw[at, pl.ds(0, HALF)] * live
        own_0[at, pl.ds(HALF, HALF)] = raw[at, pl.ds(HALF, HALF)] * live

    def build(g, carry):
        slots = [g * GROUP + step for step in range(GROUP)]
        found = [(column(fields[pl.ds(k, 1)], eye), column(noisy_ref[pl.ds(k, 1)], eye)) for k in slots]
        for k, (packed, noise) in zip(slots, found):
            build_slot(k, packed, noise)
        for k in slots:
            gather_slot(0, k)
        return carry

    lax.fori_loop(0, SLOTS // GROUP, build, 0)

    for load in loads[8:]:
        load.wait()
    for l in range(LAYERS):
        edge_w[l] = edge_w[l] * jnp.asarray(0.25 / 2**l, BF16)

    def project(nodes, l):
        values = dot(nodes, nbr_w[l])
        return jnp.concatenate([values[:, :WIDTH] * 0.5, values[:, WIDTH:]], axis=1).astype(BF16)

    for l in range(LAYERS):
        def pick_own(ch, carry, l=l):
            at = pl.ds(pl.multiple_of(ch * CHUNK, CHUNK), CHUNK)
            picked = dot(pick[at, pl.ds(FAR, PICK - FAR)], picked_from[pl.ds(FAR, PICK - FAR)])
            pre_part[at] = picked[:, :WIDTH]
            messages[at] = picked[:, WIDTH:]
            for step in range(CHUNK // CITIES):
                gather_slot(l, ch * (CHUNK // CITIES) + step)
            return carry

        nodes = hist[l]
        own = dot(nodes, own_w[l])
        high, low = split(0.5 * (own[:, :WIDTH] + time_rows[pl.ds(8 * l, 1)]))
        picked_from[pl.ds(576, 64), pl.ds(0, WIDTH)] = high.astype(BF16)
        picked_from[pl.ds(640, 64), pl.ds(0, WIDTH)] = low.astype(BF16)
        picked_from[pl.ds(512, 64)] = project(nodes, l)
        if l > 0:
            lax.fori_loop(0, CHUNKS, pick_own, 0)
        for d in range(8):
            node_copy(l, d, node_ref).wait_recv()
        picked_from[pl.ds(0, 512)] = project(nodes_in[l], l)
        for d in range(8):
            edge_copy(l, d).wait_recv()

        def multiply(ch, l=l):
            start = pl.multiple_of(ch * CHUNK, CHUNK)
            at = pl.ds(start, CHUNK)
            mine = own_0[at].astype(F32) if l == 0 else halves(wides[l], start, CHUNK)
            both = mine + halves(gathered, start, CHUNK) + dot(reach[at], edges_in[l])
            both_buf[...] = both
            depth = PICK if l == 0 else FAR
            picked = dot(pick[at, pl.ds(0, depth)], picked_from[pl.ds(0, depth)])
            pre = picked[:, :WIDTH] + dot(both.astype(BF16), edge_w[l])
            message = picked[:, WIDTH:]
            pre_buf[...] = pre if l == 0 else pre + pre_part[at]
            message_buf[...] = message if l == 0 else message + messages[at]

        def apply(ch, total, l=l):
            start = pl.multiple_of(ch * CHUNK, CHUNK)
            pre = pre_buf[...]
            message = message_buf[...]
            gated = message + jnp.tanh(pre) * message
            total = total + jnp.sum(gated.reshape(CHUNK // CITIES, CITIES, WIDTH), axis=0)
            centered = pre - jnp.mean(pre, axis=-1, keepdims=True)
            spread = jnp.sum(centered * centered, axis=-1, keepdims=True)
            scale = lax.rsqrt(spread + 0.25e-05 * WIDTH) * (WIDTH**0.5 * 2 ** (l + 1))
            following = both_buf[...] + jnp.maximum(centered * scale, 0.0)
            if l + 1 < LAYERS:
                put_halves(wides[l + 1], start, following)
            else:
                own_3[pl.ds(start, CHUNK)] = (following * 0.5 ** (l + 1)).astype(BF16)
            return total

        def overlap(ch, total):
            total = apply(ch - 1, total)
            multiply(ch)
            return total

        multiply(0)
        total = lax.fori_loop(1, CHUNKS, overlap, jnp.zeros((CITIES, WIDTH), F32))
        total = apply(CHUNKS - 1, total)
        update = jnp.maximum(norm(own[:, WIDTH:] + 0.5 * total), 0.0)
        hist[l + 1] = (nodes.astype(F32) + update).astype(BF16)
        if l + 1 < LAYERS:
            send_exchange(l + 1)

    store = pltpu.make_async_copy(own_3, edge_out, copy_sem.at[0])
    store.start()
    node_out[...] = hist[LAYERS]

    def drain(l, carry):
        for d in range(8):
            node_copy(l, d, node_ref).wait_send()
            edge_copy(l, d).wait_send()
        return carry

    lax.fori_loop(0, LAYERS, drain, 0)
    store.wait()


def by_slot(row):
    city = row // SLOTS
    return (row - city * SLOTS) * CITIES + city


def in_hbm(array):
    return pltpu.with_memory_space_constraint(array, pltpu.HBM)


def on_device(
    grid_y,
    grid_x,
    node_state,
    edge_state,
    noisy_edges,
    timestep,
    neighbors,
    mirror_src,
    send_rows,
    node_own,
    node_nbr,
    edge_weight,
    noise_embed,
    time_embed,
    time_layer,
):
    half = WIDTH // 2
    frequency = jnp.exp(-math.log(10000.0) * jnp.arange(half, dtype=F32) / half)
    phases = timestep[0].astype(F32) * frequency
    embedding = jnp.concatenate([jnp.cos(phases), jnp.sin(phases)])[None, :]
    embedding = jnp.broadcast_to(embedding, (8, WIDTH))
    edge_rows = jnp.transpose(edge_state, (1, 0, 2)).reshape(ROWS, WIDTH)
    vmem = pl.BlockSpec(memory_space=pltpu.VMEM)
    hbm = pl.BlockSpec(memory_space=pltpu.HBM)
    smem = pl.BlockSpec(memory_space=pltpu.SMEM)
    nbr, mirror = neighbors.T, mirror_src.T
    itself = jnp.arange(ROWS, dtype=jnp.int32).reshape(SLOTS, CITIES)
    partner_at = jnp.where(mirror >= 0, jnp.where(mirror >= ROWS, ROWS, by_slot(mirror)), itself)
    row_at = jnp.where(nbr >= 0, partner_at, ROWS) * 2
    send_at = jnp.where(send_rows[0] >= 0, by_slot(send_rows[0]), ROWS) * 2
    node_out, edge_out = pl.pallas_call(
        functools.partial(kernel, grid_y, grid_x),
        out_shape=(
            jax.ShapeDtypeStruct((CITIES, WIDTH), BF16),
            jax.ShapeDtypeStruct((ROWS, WIDTH), BF16),
        ),
        in_specs=[hbm] * 5 + [smem] * 2 + [hbm] * 4 + [vmem] + [hbm] * 2,
        out_specs=(vmem, pl.BlockSpec(memory_space=pl.ANY)),
        scratch_shapes=[
            pltpu.VMEM((CITIES, WIDTH), BF16),
            pltpu.VMEM((SLOTS, CITIES), F32),
            pltpu.VMEM((SLOTS, CITIES), jnp.int32),
            pltpu.VMEM((SLOTS, CITIES), jnp.int32),
            pltpu.VMEM((1, WIDTH), F32),
            pltpu.VMEM((LAYERS, WIDTH, 2 * WIDTH), BF16),
            pltpu.VMEM((LAYERS, WIDTH, 2 * WIDTH), BF16),
            pltpu.VMEM((LAYERS, WIDTH, WIDTH), BF16),
            pltpu.VMEM((WIDTH, WIDTH), F32),
            pltpu.VMEM((LAYERS, WIDTH, WIDTH), F32),
            pltpu.VMEM((ROWS, WIDTH), BF16),
        ]
        + [pltpu.VMEM((ROWS, WIDTH), BF16)] * 2
        + [pltpu.VMEM((2 * ROWS + 8, HALF), F32)] * 3
        + [
            pltpu.VMEM((2 * ROWS, HALF), F32),
            pltpu.VMEM((ROWS, PICK), BF16),
            pltpu.VMEM((ROWS, INCOMING), BF16),
            pltpu.VMEM((PICK, 2 * WIDTH), BF16),
            pltpu.VMEM((ROWS, WIDTH), F32),
            pltpu.VMEM((ROWS, WIDTH), F32),
        ]
        + [pltpu.VMEM((CHUNK, WIDTH), F32)] * 3
        + [
            pltpu.VMEM((SLOTS, CITIES), F32),
            pltpu.VMEM((2 * INCOMING, HALF), F32),
            pltpu.VMEM((8 * LAYERS, WIDTH), F32),
            pltpu.VMEM((LAYERS + 1, CITIES, WIDTH), BF16),
            pltpu.VMEM((LAYERS, 8 * CITIES, WIDTH), BF16),
            pltpu.VMEM((LAYERS, INCOMING, WIDTH), BF16),
            pltpu.VMEM((LAYERS, INCOMING, WIDTH), BF16),
            pltpu.SemaphoreType.DMA((LAYERS, 16)),
            pltpu.SemaphoreType.DMA((LAYERS, 16)),
            pltpu.SemaphoreType.DMA((11,)),
        ],
        compiler_params=pltpu.CompilerParams(
            collective_id=0, has_side_effects=True, vmem_limit_bytes=48 * 1024 * 1024
        ),
    )(
        *map(
            in_hbm,
            (
                node_state,
                edge_rows,
                noisy_edges.T,
                nbr,
                mirror,
            ),
        ),
        row_at,
        send_at,
        *map(in_hbm, (node_own, node_nbr, edge_weight, noise_embed[None, :])),
        embedding,
        in_hbm(time_embed),
        in_hbm(time_layer),
    )
    edge_out = edge_out.reshape(SLOTS, CITIES, WIDTH)
    return (node_out, jnp.transpose(edge_out, (1, 0, 2)))


def solution(mesh):
    rows = P(("ty", "tx"), None)
    cubes = P(("ty", "tx"), None, None)
    return jax.shard_map(
        functools.partial(on_device, mesh.shape["ty"], mesh.shape["tx"]),
        mesh=mesh,
        in_specs=(rows, cubes, rows, P(), rows, rows, cubes) + (P(),) * 6,
        out_specs=(rows, cubes),
        check_vma=False,
    )
```

```python
import functools
import math

import jax
import jax.numpy as jnp
from jax import lax
from jax.experimental import pallas as pl
from jax.experimental.pallas import tpu as pltpu
from jax.sharding import PartitionSpec as P

LAYERS = 3
CITIES = 64
SLOTS = 50
WIDTH = 256
HALF = 128
ROWS = CITIES * SLOTS
CAP = 16
INCOMING = 8 * CAP
PICK = 768
PART = 16
CHUNK = PART * SLOTS
CHUNKS = ROWS // CHUNK
GROUP = 2
FAR = 512
EARLY = 640
MESH = pl.DeviceIdType.MESH
F32 = jnp.float32
BF16 = jnp.bfloat16
OFFSETS = [(y, x) for y in (-1, 0, 1) for x in (-1, 0, 1) if (y, x) != (0, 0)]


def norm(values, epsilon=1e-05):
    centered = values - jnp.mean(values, axis=-1, keepdims=True)
    spread = jnp.mean(centered * centered, axis=-1, keepdims=True)
    return centered * lax.rsqrt(spread + epsilon)


def split(values):
    high = values.astype(BF16).astype(F32)
    return high, values - high


def dot(a, b):
    return jnp.dot(a, b, preferred_element_type=F32)


def exact_dot(a, b):
    return jnp.dot(a, b, precision=lax.Precision.HIGHEST, preferred_element_type=F32)


def column(row, eye):
    return jnp.sum(jnp.where(eye, jnp.broadcast_to(row, eye.shape), 0.0), axis=1, keepdims=True)


def halves(ref, start, count):
    left = ref[pl.ds(start * 2, count, stride=2), :]
    right = ref[pl.ds(start * 2 + 1, count, stride=2), :]
    return jnp.concatenate([left, right], axis=1)


def put_halves(ref, start, values):
    count = values.shape[0]
    ref[pl.ds(start * 2, count, stride=2), :] = values[:, :HALF]
    ref[pl.ds(start * 2 + 1, count, stride=2), :] = values[:, HALF:]


def kernel(
    grid_y,
    grid_x,
    node_hbm,
    edge_hbm,
    noisy_hbm,
    nbr_ids_hbm,
    mirror_hbm,
    row_at,
    own_hbm,
    nbr_hbm,
    edge_w_hbm,
    noise_hbm,
    emb_ref,
    time_embed_hbm,
    time_layer_hbm,
    node_out,
    edge_out,
    node_ref,
    noisy_ref,
    nbr_ref,
    mirror_ref,
    noise_ref,
    own_w,
    nbr_w,
    edge_w,
    time_embed,
    time_layer,
    raw,
    own_0,
    own_3,
    wide_0,
    wide_1,
    wide_2,
    gathered,
    pick,
    reach,
    picked_from,
    pre_part,
    messages,
    pre_buf,
    message_buf,
    both_buf,
    own_buf,
    fields,
    sent_wide,
    time_rows,
    hist,
    nodes_in,
    edges_in,
    edges_sent,
    send_sem,
    recv_sem,
    copy_sem,
):
    wides = [wide_0, wide_1, wide_2]
    here_y = lax.axis_index("ty")
    here_x = lax.axis_index("tx")
    targets = [
        (lax.rem(here_y - y + grid_y, grid_y), lax.rem(here_x - x + grid_x, grid_x))
        for y, x in OFFSETS
    ]
    barrier = pltpu.get_barrier_semaphore()
    for target in targets:
        pl.semaphore_signal(barrier, inc=1, device_id=target, device_id_type=MESH)

    pairs = [
        (nbr_ids_hbm, nbr_ref),
        (mirror_hbm, mirror_ref),
        (noise_hbm, noise_ref),
        (node_hbm, node_ref),
        (noisy_hbm, noisy_ref),
        (edge_hbm, raw),
        (time_embed_hbm, time_embed),
        (time_layer_hbm, time_layer),
        (own_hbm, own_w),
        (nbr_hbm, nbr_w),
        (edge_w_hbm, edge_w),
    ]
    loads = [pltpu.make_async_copy(s, t, copy_sem.at[i]) for i, (s, t) in enumerate(pairs)]
    for load in loads:
        load.start()
    for load in loads[:5]:
        load.wait()

    def node_copy(layer, d, part=0):
        start, count, source = (0, CITIES, node_ref) if layer == 0 else (part * PART, PART, hist.at[layer])
        start = pl.multiple_of(start, count)
        return pltpu.make_async_remote_copy(
            src_ref=source.at[pl.ds(start, count)],
            dst_ref=nodes_in.at[layer, pl.ds(d * CITIES + start, count)],
            send_sem=send_sem.at[layer, 0],
            recv_sem=recv_sem.at[layer, 0],
            device_id=targets[d],
            device_id_type=MESH,
        )

    def edge_copy(layer, d):
        return pltpu.make_async_remote_copy(
            src_ref=edges_sent.at[layer, pl.ds(d * CAP, CAP)],
            dst_ref=edges_in.at[layer, pl.ds(d * CAP, CAP)],
            send_sem=send_sem.at[layer, 1],
            recv_sem=recv_sem.at[layer, 1],
            device_id=targets[d],
            device_id_type=MESH,
        )

    def all_copies(layer, kind):
        block = (nodes_in, edges_in)[kind].at[layer]
        return pltpu.make_async_remote_copy(
            src_ref=block,
            dst_ref=block,
            send_sem=send_sem.at[layer, kind],
            recv_sem=recv_sem.at[layer, kind],
            device_id=targets[0],
            device_id_type=MESH,
        )

    nbr = nbr_ref[...]
    valid = nbr >= 0
    safe = jnp.maximum(nbr, 0)
    tile = safe >> 6
    rel = ((tile >> 4) - here_y + 1) * 3 + (tile & 15) - here_x + 1
    block = jnp.where(rel < 4, rel, jnp.where(rel == 4, 8, rel - 1))
    pick_at = jnp.where(valid, block * CITIES + (safe & 63), -1)
    mirror = mirror_ref[...]
    came = (mirror - ROWS) >> 4
    came = came + jnp.where(came >= 4, 1, 0)
    came_y = (came * 11) >> 5
    from_y = here_y + came_y - 1
    from_x = here_x + (came - 3 * came_y) - 1
    inside = (from_y >= 0) & (from_y < grid_y) & (from_x >= 0) & (from_x < grid_x)
    is_far = mirror >= ROWS
    far_at = jnp.where(valid & is_far & inside, mirror - ROWS, -1)
    fields[...] = ((far_at + 1) + (pick_at + 1) * 256).astype(F32)
    hist[0] = node_ref[...]
    for wide in wides:
        wide[pl.ds(2 * ROWS, 8)] = jnp.zeros((8, HALF), F32)
    noise_high, noise_low = split(0.5 * noise_ref[...])
    which = lax.broadcasted_iota(jnp.int32, (CITIES, WIDTH), 0)
    noise_rows = jnp.where(which < 2, noise_high, jnp.where(which == 2, noise_low, 0.0))
    picked_from[pl.ds(704, 64), pl.ds(0, WIDTH)] = noise_rows.astype(BF16)
    picked_from[pl.ds(576, 192), pl.ds(WIDTH, WIDTH)] = jnp.zeros((192, WIDTH), BF16)

    loads[5].wait()

    def widen(g, carry):
        for step in range(GROUP):
            k = g * GROUP + step
            values = raw[pl.ds(pl.multiple_of(k * CITIES, CITIES), CITIES)].astype(F32)
            for part in range(CHUNKS):
                put_halves(wide_0, part * CHUNK + k * PART, values[part * PART : (part + 1) * PART])
        return carry

    lax.fori_loop(0, SLOTS // GROUP, widen, 0)
    def send_exchange(l):
        for d in range(8):
            for p in range(CAP):
                at = row_at[SLOTS + d, p]
                to = (d * CAP + p) * 2
                sent_wide[pl.ds(to, 1), :] = wides[l][pl.ds(at, 1), :]
                sent_wide[pl.ds(to + 1, 1), :] = wides[l][pl.ds(at + 1, 1), :]
        if l > 0:
            for d in range(8):
                node_copy(l, d, CHUNKS - 1).start()
        edges_sent[l] = halves(sent_wide, 0, INCOMING).astype(BF16)
        for d in range(8):
            edge_copy(l, d).start()

    pl.semaphore_wait(barrier, 8)
    for d in range(8):
        node_copy(0, d).start()
    send_exchange(0)
    loads[6].wait()
    loads[7].wait()
    hidden = jnp.maximum(exact_dot(emb_ref[...], time_embed[...]), 0.0)
    for l in range(LAYERS):
        time_rows[pl.ds(8 * l, 8)] = exact_dot(hidden, time_layer[l])


    def gather_part(l, k, part, first):
        for c in range(PART):
            at = row_at[k, part * PART + c]
            to = first + 2 * c
            gathered[pl.ds(to, 1), :] = wides[l][pl.ds(at, 1), :]
            gathered[pl.ds(to + 1, 1), :] = wides[l][pl.ds(at + 1, 1), :]

    def gather_slot(l, k):
        for part in range(CHUNKS):
            gather_part(l, k, part, 2 * (part * CHUNK + k * PART))

    eye = lax.broadcasted_iota(jnp.int32, (CITIES, CITIES), 1)
    eye = eye == lax.broadcasted_iota(jnp.int32, (CITIES, CITIES), 0)
    lanes = lax.broadcasted_iota(jnp.int32, (CITIES, HALF), 1)
    rows = lax.broadcasted_iota(jnp.int32, (CITIES, HALF), 0)
    zero = jnp.zeros((CITIES, HALF), BF16)

    def build_slot(k, packed, noise):
        at = pl.ds(pl.multiple_of(k * CITIES, CITIES), CITIES)
        start = pl.multiple_of(k * PART, PART)

        def put(ref, column, values):
            for part in range(CHUNKS):
                to = pl.ds(part * CHUNK + start, PART)
                ref[to, pl.ds(column, HALF)] = values[part * PART : (part + 1) * PART]

        packed = jnp.broadcast_to(packed.astype(jnp.int32), (CITIES, HALF))
        pick_at = (packed >> 8) - 1
        far_at = (packed & 255) - 1
        live = jnp.where(pick_at >= 0, 1.0, 0.0)
        put(reach, 0, jnp.where(lanes == far_at, 1.0, 0.0).astype(BF16))
        low = jnp.where(lanes == (pick_at & 127), 1.0, 0.0).astype(BF16)
        high = (pick_at >> 7).astype(F32).astype(BF16)
        hots = [jnp.where(high == jnp.asarray(t, BF16), low, zero) for t in range(5)]
        for t in range(4):
            put(pick, t * HALF, hots[t])
        own = jnp.where(lanes == rows + CITIES, live, 0.0)
        put(pick, 512, hots[4] + own.astype(BF16))
        noise_high, noise_low = split(noise * live)
        rest = jnp.where(lanes == rows, live, 0.0)
        rest = jnp.where((lanes == 64) | (lanes == 66), noise_high, rest)
        rest = jnp.where(lanes == 65, noise_low, rest)
        put(pick, 640, rest.astype(BF16))
        live = live.astype(BF16)
        put(own_0, 0, raw[at, pl.ds(0, HALF)] * live)
        put(own_0, HALF, raw[at, pl.ds(HALF, HALF)] * live)

    def build(g, carry):
        slots = [g * GROUP + step for step in range(GROUP)]
        found = [(column(fields[pl.ds(k, 1)], eye), column(noisy_ref[pl.ds(k, 1)], eye)) for k in slots]
        for k, (packed, noise) in zip(slots, found):
            build_slot(k, packed, noise)
        for k in slots:
            gather_slot(0, k)
        return carry

    lax.fori_loop(0, SLOTS // GROUP, build, 0)

    for load in loads[8:]:
        load.wait()
    for l in range(LAYERS):
        edge_w[l] = edge_w[l] * jnp.asarray(0.25 / 2**l, BF16)

    def project(nodes, l):
        values = dot(nodes, nbr_w[l])
        return jnp.concatenate([values[:, :WIDTH] * 0.5, values[:, WIDTH:]], axis=1).astype(BF16)

    for l in range(LAYERS):
        def pick_own(ch, carry, l=l):
            at = pl.ds(pl.multiple_of(ch * EARLY, EARLY), EARLY)
            picked = dot(pick[at, pl.ds(FAR, PICK - FAR)], picked_from[pl.ds(FAR, PICK - FAR)])
            pre_part[at] = picked[:, :WIDTH]
            messages[at] = picked[:, WIDTH:]
            for step in range(EARLY // CITIES):
                gather_slot(l, ch * (EARLY // CITIES) + step)
            return carry

        nodes = hist[l]
        own = dot(nodes, own_w[l])
        own_buf[...] = own[:, WIDTH:]
        high, low = split(0.5 * (own[:, :WIDTH] + time_rows[pl.ds(8 * l, 1)]))
        picked_from[pl.ds(576, 64), pl.ds(0, WIDTH)] = high.astype(BF16)
        picked_from[pl.ds(640, 64), pl.ds(0, WIDTH)] = low.astype(BF16)
        picked_from[pl.ds(512, 64)] = project(nodes, l)
        if l > 0:
            lax.fori_loop(0, ROWS // EARLY, pick_own, 0)
        all_copies(l, 0).wait_recv()
        picked_from[pl.ds(0, 512)] = project(nodes_in[l], l)
        all_copies(l, 1).wait_recv()

        def multiply(ch, l=l):
            start = pl.multiple_of(ch * CHUNK, CHUNK)
            at = pl.ds(start, CHUNK)
            mine = own_0[at].astype(F32) if l == 0 else halves(wides[l], start, CHUNK)
            both = mine + halves(gathered, start, CHUNK) + dot(reach[at], edges_in[l])
            both_buf[...] = both
            depth = PICK if l == 0 else FAR
            picked = dot(pick[at, pl.ds(0, depth)], picked_from[pl.ds(0, depth)])
            pre = picked[:, :WIDTH] + dot(both.astype(BF16), edge_w[l])
            message = picked[:, WIDTH:]
            pre_buf[...] = pre if l == 0 else pre + pre_part[at]
            message_buf[...] = message if l == 0 else message + messages[at]

        def apply(ch, l=l):
            start = pl.multiple_of(ch * CHUNK, CHUNK)
            pre = pre_buf[...]
            message = message_buf[...]
            gated = message + jnp.tanh(pre) * message
            total = jnp.sum(gated.reshape(SLOTS, PART, WIDTH), axis=0)
            centered = pre - jnp.mean(pre, axis=-1, keepdims=True)
            spread = jnp.sum(centered * centered, axis=-1, keepdims=True)
            scale = lax.rsqrt(spread + 0.25e-05 * WIDTH) * (WIDTH**0.5 * 2 ** (l + 1))
            following = both_buf[...] + jnp.maximum(centered * scale, 0.0)
            if l + 1 < LAYERS:
                put_halves(wides[l + 1], start, following)
            else:
                following = (following * 0.5 ** (l + 1)).astype(BF16)
                for k in range(SLOTS):
                    to = pl.multiple_of(k * CITIES + ch * PART, PART)
                    own_3[pl.ds(to, PART)] = following[k * PART : (k + 1) * PART]
            cities = pl.ds(pl.multiple_of(ch * PART, PART), PART)
            update = jnp.maximum(norm(own_buf[cities] + 0.5 * total), 0.0)
            hist[l + 1, cities] = (hist[l, cities].astype(F32) + update).astype(BF16)

        def overlap(ch, carry, l=l):
            apply(ch - 1)
            multiply(ch)
            if l + 1 < LAYERS:
                for d in range(8):
                    node_copy(l + 1, d, ch - 1).start()
            return carry

        multiply(0)
        lax.fori_loop(1, CHUNKS, overlap, 0)
        apply(CHUNKS - 1)
        if l + 1 < LAYERS:
            send_exchange(l + 1)

    store = pltpu.make_async_copy(own_3, edge_out, copy_sem.at[0])
    store.start()
    node_out[...] = hist[LAYERS]

    for l in range(LAYERS):
        all_copies(l, 0).wait_send()
        all_copies(l, 1).wait_send()
    store.wait()


def row_of(slot, city):
    return (city >> 4) * CHUNK + slot * PART + (city & (PART - 1))


def by_slot(row):
    city = (row * 5243) >> 18
    return row_of(row - city * SLOTS, city)


def in_hbm(array):
    return pltpu.with_memory_space_constraint(array, pltpu.HBM)


def on_device(
    grid_y,
    grid_x,
    node_state,
    edge_state,
    noisy_edges,
    timestep,
    neighbors,
    mirror_src,
    send_rows,
    node_own,
    node_nbr,
    edge_weight,
    noise_embed,
    time_embed,
    time_layer,
):
    half = WIDTH // 2
    frequency = jnp.exp(-math.log(10000.0) * jnp.arange(half, dtype=F32) / half)
    phases = timestep[0].astype(F32) * frequency
    embedding = jnp.concatenate([jnp.cos(phases), jnp.sin(phases)])[None, :]
    embedding = jnp.broadcast_to(embedding, (8, WIDTH))
    edge_rows = jnp.transpose(edge_state, (1, 0, 2)).reshape(ROWS, WIDTH)
    vmem = pl.BlockSpec(memory_space=pltpu.VMEM)
    hbm = pl.BlockSpec(memory_space=pltpu.HBM)
    smem = pl.BlockSpec(memory_space=pltpu.SMEM)
    nbr, mirror = neighbors.T, mirror_src.T
    slot = lax.broadcasted_iota(jnp.int32, (SLOTS, CITIES), 0)
    itself = row_of(slot, lax.broadcasted_iota(jnp.int32, (SLOTS, CITIES), 1))
    partner_at = jnp.where(mirror >= 0, jnp.where(mirror >= ROWS, ROWS, by_slot(mirror)), itself)
    row_at = jnp.where(nbr >= 0, partner_at, ROWS) * 2
    send_at = jnp.where(send_rows[0] >= 0, by_slot(send_rows[0]), ROWS) * 2
    row_at = jnp.concatenate([row_at, jnp.pad(send_at, ((0, 0), (0, CITIES - CAP)))])
    node_out, edge_out = pl.pallas_call(
        functools.partial(kernel, grid_y, grid_x),
        out_shape=(
            jax.ShapeDtypeStruct((CITIES, WIDTH), BF16),
            jax.ShapeDtypeStruct((ROWS, WIDTH), BF16),
        ),
        in_specs=[hbm] * 5 + [smem] + [hbm] * 4 + [vmem] + [hbm] * 2,
        out_specs=(vmem, pl.BlockSpec(memory_space=pl.ANY)),
        scratch_shapes=[
            pltpu.VMEM((CITIES, WIDTH), BF16),
            pltpu.VMEM((SLOTS, CITIES), F32),
            pltpu.VMEM((SLOTS, CITIES), jnp.int32),
            pltpu.VMEM((SLOTS, CITIES), jnp.int32),
            pltpu.VMEM((1, WIDTH), F32),
            pltpu.VMEM((LAYERS, WIDTH, 2 * WIDTH), BF16),
            pltpu.VMEM((LAYERS, WIDTH, 2 * WIDTH), BF16),
            pltpu.VMEM((LAYERS, WIDTH, WIDTH), BF16),
            pltpu.VMEM((WIDTH, WIDTH), F32),
            pltpu.VMEM((LAYERS, WIDTH, WIDTH), F32),
            pltpu.VMEM((ROWS, WIDTH), BF16),
        ]
        + [pltpu.VMEM((ROWS, WIDTH), BF16)] * 2
        + [pltpu.VMEM((2 * ROWS + 8, HALF), F32)] * 3
        + [
            pltpu.VMEM((2 * ROWS, HALF), F32),
            pltpu.VMEM((ROWS, PICK), BF16),
            pltpu.VMEM((ROWS, INCOMING), BF16),
            pltpu.VMEM((PICK, 2 * WIDTH), BF16),
            pltpu.VMEM((ROWS, WIDTH), F32),
            pltpu.VMEM((ROWS, WIDTH), F32),
        ]
        + [pltpu.VMEM((CHUNK, WIDTH), F32)] * 3
        + [
            pltpu.VMEM((CITIES, WIDTH), F32),
            pltpu.VMEM((SLOTS, CITIES), F32),
            pltpu.VMEM((2 * INCOMING, HALF), F32),
            pltpu.VMEM((8 * LAYERS, WIDTH), F32),
            pltpu.VMEM((LAYERS + 1, CITIES, WIDTH), BF16),
            pltpu.VMEM((LAYERS, 8 * CITIES, WIDTH), BF16),
            pltpu.VMEM((LAYERS, INCOMING, WIDTH), BF16),
            pltpu.VMEM((LAYERS, INCOMING, WIDTH), BF16),
            pltpu.SemaphoreType.DMA((LAYERS, 2)),
            pltpu.SemaphoreType.DMA((LAYERS, 2)),
            pltpu.SemaphoreType.DMA((11,)),
        ],
        compiler_params=pltpu.CompilerParams(
            collective_id=0, has_side_effects=True, vmem_limit_bytes=48 * 1024 * 1024
        ),
    )(
        *map(
            in_hbm,
            (
                node_state,
                edge_rows,
                noisy_edges.T,
                nbr,
                mirror,
            ),
        ),
        row_at,
        *map(in_hbm, (node_own, node_nbr, edge_weight, noise_embed[None, :])),
        embedding,
        in_hbm(time_embed),
        in_hbm(time_layer),
    )
    edge_out = edge_out.reshape(SLOTS, CITIES, WIDTH)
    return (node_out, jnp.transpose(edge_out, (1, 0, 2)))


def solution(mesh):
    rows = P(("ty", "tx"), None)
    cubes = P(("ty", "tx"), None, None)
    return jax.shard_map(
        functools.partial(on_device, mesh.shape["ty"], mesh.shape["tx"]),
        mesh=mesh,
        in_specs=(rows, cubes, rows, P(), rows, rows, cubes) + (P(),) * 6,
        out_specs=(rows, cubes),
        check_vma=False,
    )
```

```python
import functools
import math

import jax
import jax.numpy as jnp
from jax import lax
from jax.experimental import pallas as pl
from jax.experimental.pallas import tpu as pltpu
from jax.sharding import PartitionSpec as P

LAYERS = 3
CITIES = 64
SLOTS = 50
WIDTH = 256
HALF = 128
ROWS = CITIES * SLOTS
CAP = 16
INCOMING = 8 * CAP
PICK = 768
PART = 16
CHUNK = PART * SLOTS
CHUNKS = ROWS // CHUNK
GROUP = 2
FAR = 512
EARLY = 640
MESH = pl.DeviceIdType.MESH
F32 = jnp.float32
BF16 = jnp.bfloat16
OFFSETS = [(y, x) for y in (-1, 0, 1) for x in (-1, 0, 1) if (y, x) != (0, 0)]


def norm(values, epsilon=1e-05):
    centered = values - jnp.mean(values, axis=-1, keepdims=True)
    spread = jnp.mean(centered * centered, axis=-1, keepdims=True)
    return centered * lax.rsqrt(spread + epsilon)


def split(values):
    high = values.astype(BF16).astype(F32)
    return high, values - high


def dot(a, b):
    return jnp.dot(a, b, preferred_element_type=F32)


def column(row, eye):
    return jnp.sum(jnp.where(eye, jnp.broadcast_to(row, eye.shape), 0.0), axis=1, keepdims=True)


def halves(ref, start, count):
    left = ref[pl.ds(start * 2, count, stride=2), :]
    right = ref[pl.ds(start * 2 + 1, count, stride=2), :]
    return jnp.concatenate([left, right], axis=1)


def put_halves(ref, start, values):
    count = values.shape[0]
    ref[pl.ds(start * 2, count, stride=2), :] = values[:, :HALF]
    ref[pl.ds(start * 2 + 1, count, stride=2), :] = values[:, HALF:]


def row_of(slot, city):
    return (city >> 4) * CHUNK + slot * PART + (city & (PART - 1))


def by_slot(row):
    city = (row * 5243) >> 18
    return row_of(row - city * SLOTS, city)


def kernel(
    grid_y,
    grid_x,
    node_hbm,
    edge_hbm,
    noisy_hbm,
    nbr_ids_hbm,
    mirror_hbm,
    send_hbm,
    own_hbm,
    nbr_hbm,
    edge_w_hbm,
    noise_hbm,
    emb_ref,
    time_embed_hbm,
    time_layer_hbm,
    node_out,
    edge_out,
    node_ref,
    noisy_ref,
    nbr_ref,
    mirror_ref,
    send_ref,
    noise_ref,
    own_w,
    nbr_w,
    edge_w,
    time_embed,
    time_layer,
    raw,
    own_0,
    own_3,
    wide_0,
    wide_1,
    wide_2,
    gathered,
    pick,
    reach,
    picked_from,
    pre_part,
    messages,
    pre_buf,
    message_buf,
    both_buf,
    own_buf,
    fields,
    row_table,
    send_table,
    row_at,
    send_at,
    sent_wide,
    time_rows,
    hist,
    nodes_in,
    edges_in,
    edges_sent,
    send_sem,
    recv_sem,
    copy_sem,
):
    wides = [wide_0, wide_1, wide_2]
    here_y = lax.axis_index("ty")
    here_x = lax.axis_index("tx")
    targets = [
        (lax.rem(here_y - y + grid_y, grid_y), lax.rem(here_x - x + grid_x, grid_x))
        for y, x in OFFSETS
    ]
    barrier = pltpu.get_barrier_semaphore()
    for target in targets:
        pl.semaphore_signal(barrier, inc=1, device_id=target, device_id_type=MESH)

    pairs = [
        (nbr_ids_hbm, nbr_ref),
        (mirror_hbm, mirror_ref),
        (send_hbm, send_ref),
        (noise_hbm, noise_ref),
        (node_hbm, node_ref),
        (noisy_hbm, noisy_ref),
        (edge_hbm, raw),
        (time_embed_hbm, time_embed),
        (time_layer_hbm, time_layer),
        (own_hbm, own_w),
        (nbr_hbm, nbr_w),
        (edge_w_hbm, edge_w),
    ]
    loads = [pltpu.make_async_copy(s, t, copy_sem.at[i]) for i, (s, t) in enumerate(pairs)]
    for load in loads:
        load.start()
    for load in loads[:6]:
        load.wait()

    def node_copy(layer, d, part=0):
        start, count, source = (0, CITIES, node_ref) if layer == 0 else (part * PART, PART, hist.at[layer])
        start = pl.multiple_of(start, count)
        return pltpu.make_async_remote_copy(
            src_ref=source.at[pl.ds(start, count)],
            dst_ref=nodes_in.at[layer, pl.ds(d * CITIES + start, count)],
            send_sem=send_sem.at[layer, 0],
            recv_sem=recv_sem.at[layer, 0],
            device_id=targets[d],
            device_id_type=MESH,
        )

    def edge_copy(layer, d):
        return pltpu.make_async_remote_copy(
            src_ref=edges_sent.at[layer, pl.ds(d * CAP, CAP)],
            dst_ref=edges_in.at[layer, pl.ds(d * CAP, CAP)],
            send_sem=send_sem.at[layer, 1],
            recv_sem=recv_sem.at[layer, 1],
            device_id=targets[d],
            device_id_type=MESH,
        )

    def all_copies(layer, kind):
        block = (nodes_in, edges_in)[kind].at[layer]
        return pltpu.make_async_remote_copy(
            src_ref=block,
            dst_ref=block,
            send_sem=send_sem.at[layer, kind],
            recv_sem=recv_sem.at[layer, kind],
            device_id=targets[0],
            device_id_type=MESH,
        )

    nbr = nbr_ref[...]
    valid = nbr >= 0
    safe = jnp.maximum(nbr, 0)
    tile = safe >> 6
    rel = ((tile >> 4) - here_y + 1) * 3 + (tile & 15) - here_x + 1
    block = jnp.where(rel < 4, rel, jnp.where(rel == 4, 8, rel - 1))
    pick_at = jnp.where(valid, block * CITIES + (safe & 63), -1)
    mirror = mirror_ref[...]
    came = (mirror - ROWS) >> 4
    came = came + jnp.where(came >= 4, 1, 0)
    came_y = (came * 11) >> 5
    from_y = here_y + came_y - 1
    from_x = here_x + (came - 3 * came_y) - 1
    inside = (from_y >= 0) & (from_y < grid_y) & (from_x >= 0) & (from_x < grid_x)
    is_far = mirror >= ROWS
    far_at = jnp.where(valid & is_far & inside, mirror - ROWS, -1)
    fields[...] = ((far_at + 1) + (pick_at + 1) * 256).astype(F32)
    slots = lax.broadcasted_iota(jnp.int32, (SLOTS, CITIES), 0)
    itself = row_of(slots, lax.broadcasted_iota(jnp.int32, (SLOTS, CITIES), 1))
    partner_at = jnp.where(mirror >= 0, jnp.where(is_far, ROWS, by_slot(mirror)), itself)
    row_table[...] = jnp.where(valid, partner_at, ROWS) * 2
    sends = send_ref[0]
    send_table[...] = jnp.where(sends >= 0, by_slot(sends), ROWS) * 2
    tables = [
        pltpu.make_async_copy(row_table, row_at, copy_sem.at[12]),
        pltpu.make_async_copy(send_table, send_at, copy_sem.at[13]),
    ]
    for table in tables:
        table.start()
    hist[0] = node_ref[...]
    for wide in wides:
        wide[pl.ds(2 * ROWS, 8)] = jnp.zeros((8, HALF), F32)
    noise_high, noise_low = split(0.5 * noise_ref[...])
    which = lax.broadcasted_iota(jnp.int32, (CITIES, WIDTH), 0)
    noise_rows = jnp.where(which < 2, noise_high, jnp.where(which == 2, noise_low, 0.0))
    picked_from[pl.ds(704, 64), pl.ds(0, WIDTH)] = noise_rows.astype(BF16)
    picked_from[pl.ds(576, 192), pl.ds(WIDTH, WIDTH)] = jnp.zeros((192, WIDTH), BF16)

    loads[6].wait()

    def widen(g, carry):
        for step in range(GROUP):
            k = g * GROUP + step
            values = raw[pl.ds(pl.multiple_of(k * CITIES, CITIES), CITIES)].astype(F32)
            for part in range(CHUNKS):
                put_halves(wide_0, part * CHUNK + k * PART, values[part * PART : (part + 1) * PART])
        return carry

    lax.fori_loop(0, SLOTS // GROUP, widen, 0)
    def send_exchange(l):
        for d in range(8):
            for p in range(CAP):
                at = send_at[d, p]
                to = (d * CAP + p) * 2
                sent_wide[pl.ds(to, 1), :] = wides[l][pl.ds(at, 1), :]
                sent_wide[pl.ds(to + 1, 1), :] = wides[l][pl.ds(at + 1, 1), :]
        if l > 0:
            for d in range(8):
                node_copy(l, d, CHUNKS - 1).start()
        edges_sent[l] = halves(sent_wide, 0, INCOMING).astype(BF16)
        for d in range(8):
            edge_copy(l, d).start()

    for table in tables:
        table.wait()
    pl.semaphore_wait(barrier, 8)
    for d in range(8):
        node_copy(0, d).start()
    send_exchange(0)
    loads[7].wait()
    loads[8].wait()
    wide_eye = lax.broadcasted_iota(jnp.int32, (WIDTH, WIDTH), 1)
    wide_eye = wide_eye == lax.broadcasted_iota(jnp.int32, (WIDTH, WIDTH), 0)
    embedded = column(emb_ref[0:1], wide_eye)
    hidden = jnp.sum(time_embed[...] * embedded, axis=0, keepdims=True)
    hidden = column(jnp.maximum(hidden, 0.0), wide_eye)
    for l in range(LAYERS):
        time_rows[pl.ds(8 * l, 1)] = jnp.sum(time_layer[l] * hidden, axis=0, keepdims=True)

    def gather_part(l, k, part, first):
        for c in range(PART):
            at = row_at[k, part * PART + c]
            to = first + 2 * c
            gathered[pl.ds(to, 1), :] = wides[l][pl.ds(at, 1), :]
            gathered[pl.ds(to + 1, 1), :] = wides[l][pl.ds(at + 1, 1), :]

    def gather_slot(l, k):
        for part in range(CHUNKS):
            gather_part(l, k, part, 2 * (part * CHUNK + k * PART))

    eye = lax.broadcasted_iota(jnp.int32, (CITIES, CITIES), 1)
    eye = eye == lax.broadcasted_iota(jnp.int32, (CITIES, CITIES), 0)
    lanes = lax.broadcasted_iota(jnp.int32, (CITIES, HALF), 1)
    rows = lax.broadcasted_iota(jnp.int32, (CITIES, HALF), 0)
    zero = jnp.zeros((CITIES, HALF), BF16)

    def build_slot(k, packed, noise):
        at = pl.ds(pl.multiple_of(k * CITIES, CITIES), CITIES)
        start = pl.multiple_of(k * PART, PART)

        def put(ref, column, values):
            for part in range(CHUNKS):
                to = pl.ds(part * CHUNK + start, PART)
                ref[to, pl.ds(column, HALF)] = values[part * PART : (part + 1) * PART]

        packed = jnp.broadcast_to(packed.astype(jnp.int32), (CITIES, HALF))
        pick_at = (packed >> 8) - 1
        far_at = (packed & 255) - 1
        live = jnp.where(pick_at >= 0, 1.0, 0.0)
        put(reach, 0, jnp.where(lanes == far_at, 1.0, 0.0).astype(BF16))
        low = jnp.where(lanes == (pick_at & 127), 1.0, 0.0).astype(BF16)
        high = (pick_at >> 7).astype(F32).astype(BF16)
        hots = [jnp.where(high == jnp.asarray(t, BF16), low, zero) for t in range(5)]
        for t in range(4):
            put(pick, t * HALF, hots[t])
        own = jnp.where(lanes == rows + CITIES, live, 0.0)
        put(pick, 512, hots[4] + own.astype(BF16))
        noise_high, noise_low = split(noise * live)
        rest = jnp.where(lanes == rows, live, 0.0)
        rest = jnp.where((lanes == 64) | (lanes == 66), noise_high, rest)
        rest = jnp.where(lanes == 65, noise_low, rest)
        put(pick, 640, rest.astype(BF16))
        live = live.astype(BF16)
        put(own_0, 0, raw[at, pl.ds(0, HALF)] * live)
        put(own_0, HALF, raw[at, pl.ds(HALF, HALF)] * live)

    def build(g, carry):
        slots = [g * GROUP + step for step in range(GROUP)]
        found = [(column(fields[pl.ds(k, 1)], eye), column(noisy_ref[pl.ds(k, 1)], eye)) for k in slots]
        for k, (packed, noise) in zip(slots, found):
            build_slot(k, packed, noise)
        for k in slots:
            gather_slot(0, k)
        return carry

    lax.fori_loop(0, SLOTS // GROUP, build, 0)

    for load in loads[9:]:
        load.wait()
    for l in range(LAYERS):
        edge_w[l] = edge_w[l] * jnp.asarray(0.25 / 2**l, BF16)

    def store(ch):
        part = pl.ds(pl.multiple_of(ch * PART, PART), PART)
        return pltpu.make_async_copy(own_3.at[:, part], edge_out.at[:, part], copy_sem.at[ch])

    def project(nodes, l):
        values = dot(nodes, nbr_w[l])
        return jnp.concatenate([values[:, :WIDTH] * 0.5, values[:, WIDTH:]], axis=1).astype(BF16)

    for l in range(LAYERS):
        def pick_own(ch, carry, l=l):
            at = pl.ds(pl.multiple_of(ch * EARLY, EARLY), EARLY)
            picked = dot(pick[at, pl.ds(FAR, PICK - FAR)], picked_from[pl.ds(FAR, PICK - FAR)])
            pre_part[at] = picked[:, :WIDTH]
            messages[at] = picked[:, WIDTH:]
            for step in range(EARLY // CITIES):
                gather_slot(l, ch * (EARLY // CITIES) + step)
            return carry

        nodes = hist[l]
        own = dot(nodes, own_w[l])
        own_buf[...] = own[:, WIDTH:]
        high, low = split(0.5 * (own[:, :WIDTH] + time_rows[pl.ds(8 * l, 1)]))
        picked_from[pl.ds(576, 64), pl.ds(0, WIDTH)] = high.astype(BF16)
        picked_from[pl.ds(640, 64), pl.ds(0, WIDTH)] = low.astype(BF16)
        picked_from[pl.ds(512, 64)] = project(nodes, l)
        if l > 0:
            lax.fori_loop(0, ROWS // EARLY, pick_own, 0)
        all_copies(l, 0).wait_recv()
        picked_from[pl.ds(0, 512)] = project(nodes_in[l], l)
        all_copies(l, 1).wait_recv()

        def multiply(ch, l=l):
            start = pl.multiple_of(ch * CHUNK, CHUNK)
            at = pl.ds(start, CHUNK)
            mine = own_0[at].astype(F32) if l == 0 else halves(wides[l], start, CHUNK)
            both = mine + halves(gathered, start, CHUNK) + dot(reach[at], edges_in[l])
            both_buf[...] = both
            depth = PICK if l == 0 else FAR
            picked = dot(pick[at, pl.ds(0, depth)], picked_from[pl.ds(0, depth)])
            pre = picked[:, :WIDTH] + dot(both.astype(BF16), edge_w[l])
            message = picked[:, WIDTH:]
            pre_buf[...] = pre if l == 0 else pre + pre_part[at]
            message_buf[...] = message if l == 0 else message + messages[at]

        def apply(ch, l=l):
            start = pl.multiple_of(ch * CHUNK, CHUNK)
            pre = pre_buf[...]
            message = message_buf[...]
            gated = message + jnp.tanh(pre) * message
            total = jnp.sum(gated.reshape(SLOTS, PART, WIDTH), axis=0)
            centered = pre - jnp.mean(pre, axis=-1, keepdims=True)
            spread = jnp.sum(centered * centered, axis=-1, keepdims=True)
            scale = lax.rsqrt(spread + 0.25e-05 * WIDTH) * (WIDTH**0.5 * 2 ** (l + 1))
            following = both_buf[...] + jnp.maximum(centered * scale, 0.0)
            if l + 1 < LAYERS:
                put_halves(wides[l + 1], start, following)
            else:
                following = (following * 0.5 ** (l + 1)).astype(BF16)
                part = pl.ds(pl.multiple_of(ch * PART, PART), PART)
                own_3[:, part, :] = following.reshape(SLOTS, PART, WIDTH)
            cities = pl.ds(pl.multiple_of(ch * PART, PART), PART)
            update = jnp.maximum(norm(own_buf[cities] + 0.5 * total), 0.0)
            hist[l + 1, cities] = (hist[l, cities].astype(F32) + update).astype(BF16)

        def overlap(ch, carry, l=l):
            apply(ch - 1)
            multiply(ch)
            if l + 1 < LAYERS:
                for d in range(8):
                    node_copy(l + 1, d, ch - 1).start()
            else:
                store(ch - 1).start()
            return carry

        multiply(0)
        lax.fori_loop(1, CHUNKS, overlap, 0)
        apply(CHUNKS - 1)
        if l + 1 < LAYERS:
            send_exchange(l + 1)

    store(CHUNKS - 1).start()
    node_out[...] = hist[LAYERS]

    for l in range(LAYERS):
        all_copies(l, 0).wait_send()
        all_copies(l, 1).wait_send()
    for part in range(CHUNKS):
        store(part).wait()


def in_hbm(array):
    return pltpu.with_memory_space_constraint(array, pltpu.HBM)


def on_device(
    grid_y,
    grid_x,
    node_state,
    edge_state,
    noisy_edges,
    timestep,
    neighbors,
    mirror_src,
    send_rows,
    node_own,
    node_nbr,
    edge_weight,
    noise_embed,
    time_embed,
    time_layer,
):
    half = WIDTH // 2
    frequency = jnp.exp(-math.log(10000.0) * jnp.arange(half, dtype=F32) / half)
    phases = timestep[0].astype(F32) * frequency
    embedding = jnp.concatenate([jnp.cos(phases), jnp.sin(phases)])[None, :]
    embedding = jnp.broadcast_to(embedding, (8, WIDTH))
    edge_rows = jnp.transpose(edge_state, (1, 0, 2)).reshape(ROWS, WIDTH)
    vmem = pl.BlockSpec(memory_space=pltpu.VMEM)
    hbm = pl.BlockSpec(memory_space=pltpu.HBM)
    node_out, edge_out = pl.pallas_call(
        functools.partial(kernel, grid_y, grid_x),
        out_shape=(
            jax.ShapeDtypeStruct((CITIES, WIDTH), BF16),
            jax.ShapeDtypeStruct((SLOTS, CITIES, WIDTH), BF16),
        ),
        in_specs=[hbm] * 10 + [vmem] + [hbm] * 2,
        out_specs=(vmem, pl.BlockSpec(memory_space=pl.ANY)),
        scratch_shapes=[
            pltpu.VMEM((CITIES, WIDTH), BF16),
            pltpu.VMEM((SLOTS, CITIES), F32),
            pltpu.VMEM((SLOTS, CITIES), jnp.int32),
            pltpu.VMEM((SLOTS, CITIES), jnp.int32),
            pltpu.VMEM((1, 8, CAP), jnp.int32),
            pltpu.VMEM((1, WIDTH), F32),
            pltpu.VMEM((LAYERS, WIDTH, 2 * WIDTH), BF16),
            pltpu.VMEM((LAYERS, WIDTH, 2 * WIDTH), BF16),
            pltpu.VMEM((LAYERS, WIDTH, WIDTH), BF16),
            pltpu.VMEM((WIDTH, WIDTH), F32),
            pltpu.VMEM((LAYERS, WIDTH, WIDTH), F32),
            pltpu.VMEM((ROWS, WIDTH), BF16),
        ]
        + [pltpu.VMEM((ROWS, WIDTH), BF16), pltpu.VMEM((SLOTS, CITIES, WIDTH), BF16)]
        + [pltpu.VMEM((2 * ROWS + 8, HALF), F32)] * 3
        + [
            pltpu.VMEM((2 * ROWS, HALF), F32),
            pltpu.VMEM((ROWS, PICK), BF16),
            pltpu.VMEM((ROWS, INCOMING), BF16),
            pltpu.VMEM((PICK, 2 * WIDTH), BF16),
            pltpu.VMEM((ROWS, WIDTH), F32),
            pltpu.VMEM((ROWS, WIDTH), F32),
        ]
        + [pltpu.VMEM((CHUNK, WIDTH), F32)] * 3
        + [
            pltpu.VMEM((CITIES, WIDTH), F32),
            pltpu.VMEM((SLOTS, CITIES), F32),
            pltpu.VMEM((SLOTS, CITIES), jnp.int32),
            pltpu.VMEM((8, CAP), jnp.int32),
            pltpu.SMEM((SLOTS, CITIES), jnp.int32),
            pltpu.SMEM((8, CAP), jnp.int32),
            pltpu.VMEM((2 * INCOMING, HALF), F32),
            pltpu.VMEM((8 * LAYERS, WIDTH), F32),
            pltpu.VMEM((LAYERS + 1, CITIES, WIDTH), BF16),
            pltpu.VMEM((LAYERS, 8 * CITIES, WIDTH), BF16),
            pltpu.VMEM((LAYERS, INCOMING, WIDTH), BF16),
            pltpu.VMEM((LAYERS, INCOMING, WIDTH), BF16),
            pltpu.SemaphoreType.DMA((LAYERS, 2)),
            pltpu.SemaphoreType.DMA((LAYERS, 2)),
            pltpu.SemaphoreType.DMA((14,)),
        ],
        compiler_params=pltpu.CompilerParams(
            collective_id=0, has_side_effects=True, vmem_limit_bytes=48 * 1024 * 1024
        ),
    )(
        *map(
            in_hbm,
            (
                node_state,
                edge_rows,
                noisy_edges.T,
                neighbors.T,
                mirror_src.T,
                send_rows,
            ),
        ),
        *map(in_hbm, (node_own, node_nbr, edge_weight, noise_embed[None, :])),
        embedding,
        in_hbm(time_embed),
        in_hbm(time_layer),
    )
    return (node_out, jnp.transpose(edge_out, (1, 0, 2)))


def solution(mesh):
    rows = P(("ty", "tx"), None)
    cubes = P(("ty", "tx"), None, None)
    return jax.shard_map(
        functools.partial(on_device, mesh.shape["ty"], mesh.shape["tx"]),
        mesh=mesh,
        in_specs=(rows, cubes, rows, P(), rows, rows, cubes) + (P(),) * 6,
        out_specs=(rows, cubes),
        check_vma=False,
    )
```
